32 devices in a mesh: gx: 4 (over x, core), gy: 4 (over z), gz: 2 (over y).
Axes of the slice: x: 2, y: 2, z: 4, core: 2. Of those that a mesh axis runs over, the one named last changes fastest.
Arguments:
- positions: float32 [3, 8, 8, 4, 128], P(None, 'gx', 'gy', 'gz'), may hold values from 0 to 1
- velocities: float32 [3, 8, 8, 4, 128], P(None, 'gx', 'gy', 'gz'), may hold values from -3 to 3
- spins: float32 [3, 8, 8, 4, 128], P(None, 'gx', 'gy', 'gz'), may hold values from -6 to 6
- radii: float32 [8, 8, 4, 128], P('gx', 'gy', 'gz'), may hold values from 0.08 to 0.13
- counts: int32 [8, 8, 4], P('gx', 'gy', 'gz'), may hold values from 16 to 128
- springs: float32 [3, 4, 8, 8, 4, 128], P(None, None, 'gx', 'gy', 'gz'), may hold values from -0.36 to 0.36
- partners: int32 [4, 8, 8, 4, 128], P(None, 'gx', 'gy', 'gz'), may hold values from -1 to 895, as said below
- cells: int32 [8, 8, 4, 128], P('gx', 'gy', 'gz'), may hold values from 0 to 16383, as said below
- departures: int32 [4, 4, 2, 6, 128], P('gx', 'gy', 'gz'), may hold values from -1 to 1023, as said below
- fluid_velocity: float32 [3, 64, 128, 512], P(None, 'gx', 'gy', 'gz'), may hold values from -6 to 6
- pressure: float32 [64, 128, 512], P('gx', 'gy', 'gz'), may hold values from -6 to 6
- pressure_source: float32 [64, 128, 512], P('gx', 'gy', 'gz'), may hold values from -6 to 6
Outputs:
- new_positions: float32 [3, 8, 8, 4, 128], P(None, 'gx', 'gy', 'gz')
- new_velocities: float32 [3, 8, 8, 4, 128], P(None, 'gx', 'gy', 'gz')
- new_spins: float32 [3, 8, 8, 4, 128], P(None, 'gx', 'gy', 'gz')
- new_springs: float32 [3, 4, 8, 8, 4, 128], P(None, None, 'gx', 'gy', 'gz')
- fluid_force: float32 [3, 64, 128, 512], P(None, 'gx', 'gy', 'gz')
- new_pressure: float32 [64, 128, 512], P('gx', 'gy', 'gz')
- arrived: float32 [4, 4, 2, 22, 6, 128], P('gx', 'gy', 'gz')
- arrived_partners: int32 [4, 4, 2, 4, 6, 128], P('gx', 'gy', 'gz')
The draws below stay inside these ranges and needn't reach their ends.
Inputs may be any that keep to these rules, and one draw needn't show every extreme that they name: `partners`: -1 marks an empty history slot; otherwise the code is bin * 128 + slot with bin 0 for the particle's own bin and 1 to 6 for the bins at -x, +x, -y, +y, -z, +z; a code never names the particle itself. The index of a cell within the particle's own bin's block of 8 x 32 // 2 x 256 // 2 cells, as in the reference program. `departures`: an entry is a local slot index ((bx * 2 + by) * 2 + bz) * 128 + slot, or -1; a slot appears at most once on its device; in each direction the used entries come first; in every draw some device fills all 128 entries of some direction.
All inputs are finite; a program needn't handle non-finite values.
Results may differ from the reference program's by a relative error of at most 0.0003.
Values sent between devices are 32-bit elements; how exact they have to be, the bound alone decides.
No kernel may reach another device: no remote copies, remote signals or barrier semaphores. Data moves between devices by JAX's collectives and lax.ppermute only.
A program may use at most 192 MiB of HBM per device.

```python
import math
import jax
import jax.numpy as jnp
from jax import lax

SLOTS = 128
HIST = 4
SUBSTEPS = 2
BX = 2
BY = 2
BZ = 2
FX = 16
FY = 32
FZ = 256
MIG = 128
GBX = 8
GBY = 8
GBZ = 4
NFX = 64
NFY = 128
NFZ = 512


def draw_partners(key, part):
    extent = (HIST, GBX, GBY, GBZ, SLOTS)
    random_keys = jax.random.split(jax.random.fold_in(key, 71), 3)
    neighbour = jax.random.randint(random_keys[0], extent, 0, 7)
    member = jax.random.randint(random_keys[1], extent, 0, SLOTS)
    itself = lax.broadcasted_iota(jnp.int32, extent, 4)
    member = jnp.where((neighbour == 0) & (member == itself), (member + 1) % SLOTS, member)
    active = jax.random.randint(random_keys[2], extent, 0, 3) > 0
    return jnp.where(active, neighbour * SLOTS + member, -1).astype(jnp.int32)


def draw_cells(key, part):
    extent = (GBX, GBY, GBZ, SLOTS)
    random_keys = jax.random.split(jax.random.fold_in(key, 83), 3)
    cell_span = (FX // BX, FY // BY, FZ // BZ)
    coords = []
    for axis_id in range(3):
        coords.append(jax.random.randint(random_keys[axis_id], extent, 0, cell_span[axis_id]))
    return ((coords[0] * cell_span[1] + coords[1]) * cell_span[2] + coords[2]).astype(jnp.int32)


def draw_departures(key, part):
    grid_x = GBX // BX
    grid_y = GBY // BY
    grid_z = GBZ // BZ
    devices_all = grid_x * grid_y * grid_z
    population = BX * BY * BZ * SLOTS
    random_keys = jax.random.split(jax.random.fold_in(key, 97), 3)
    orders = jax.vmap(lambda single: jax.random.permutation(single, population))(jax.random.split(random_keys[0], devices_all))
    chosen = orders[:, :6 * MIG].reshape(devices_all, 6, MIG).astype(jnp.int32)
    filled = jax.random.randint(random_keys[1], (devices_all, 6), 1, MIG + 1)
    busiest = jax.random.randint(random_keys[2], (), 0, devices_all * 6)
    flat_id = jnp.arange(devices_all * 6, dtype=jnp.int32).reshape(devices_all, 6)
    filled = jnp.where(flat_id == busiest, MIG, filled)
    column = lax.broadcasted_iota(jnp.int32, (devices_all, 6, MIG), 2)
    result = jnp.where(column < filled[..., None], chosen, -1)
    return result.reshape(grid_x, grid_y, grid_z, 6, MIG).astype(jnp.int32)


def place_ends(values, key, smallest, largest):
    dims = values.shape
    index_at = [jax.random.randint(jax.random.fold_in(key, axis), (), 0, dims[axis]) for axis in range(len(dims))]
    values = values.at[tuple(index_at)].set(smallest)
    longest = dims.index(max(dims))
    index_at[longest] = (index_at[longest] + 1) % dims[longest]
    return values.at[tuple(index_at)].set(largest)


def shard_levels(stream_key, shape, cuts, smallest, high):
    gain = 1.0
    for dim, parts in cuts:
        steps = jax.random.uniform(jax.random.fold_in(jax.random.fold_in(stream_key, 6), dim), (parts,), jnp.float32, smallest / len(cuts), high / len(cuts))
        gain = gain * jnp.repeat(jnp.exp(steps), shape[dim] // parts).reshape((-1,) + (1,) * (len(shape) - 1 - dim))
    return gain


def bell_draw(own_key, shape, spread, most, cuts=(), kind=jnp.bfloat16):
    values = jax.random.normal(own_key, shape, jnp.float32) * spread
    if len(cuts) > 0:
        values = shard_levels(own_key, shape, cuts, -0.22, 0.18) * values
    return jnp.clip(values, min=-most, max=most).astype(kind)


def setup_inputs(seed: int = 0) -> dict:
    arg_keys = jax.random.split(jax.random.key(seed), 13)
    positions = jnp.clip(1.0 * jax.random.uniform(arg_keys[0], (3, GBX, GBY, GBZ, SLOTS), jnp.float32) ** shard_levels(arg_keys[0], (3, GBX, GBY, GBZ, SLOTS), ((1, 4), (2, 4), (3, 2)), -0.2, 0.2), 0.0, 1.0)
    velocities = bell_draw(arg_keys[1], (3, GBX, GBY, GBZ, SLOTS), 0.5, 3.0, ((1, 4), (2, 4), (3, 2)), jnp.float32)
    spins = bell_draw(arg_keys[2], (3, GBX, GBY, GBZ, SLOTS), 1.0, 6.0, ((1, 4), (2, 4), (3, 2)), jnp.float32)
    radii = jnp.clip(0.08 + 0.049999997 * jax.random.uniform(arg_keys[3], (GBX, GBY, GBZ, SLOTS), jnp.float32) ** shard_levels(arg_keys[3], (GBX, GBY, GBZ, SLOTS), ((0, 4), (1, 4), (2, 2)), -0.2, 0.2), 0.08, 0.13)
    counts = place_ends(jax.random.randint(arg_keys[4], (GBX, GBY, GBZ), SLOTS // 8, SLOTS + 1), jax.random.fold_in(arg_keys[4], 1), SLOTS // 8, SLOTS).astype(jnp.int32)
    springs = bell_draw(arg_keys[5], (3, HIST, GBX, GBY, GBZ, SLOTS), 0.06, 0.36, ((2, 4), (3, 4), (4, 2)), jnp.float32)
    partners = draw_partners(jax.random.fold_in(arg_keys[12], 71), 0)
    cells = draw_cells(jax.random.fold_in(arg_keys[12], 71), 0)
    departures = draw_departures(jax.random.fold_in(arg_keys[12], 71), 0)
    fluid_velocity = bell_draw(arg_keys[9], (3, NFX, NFY, NFZ), 1.0, 6.0, ((1, 4), (2, 4), (3, 2)), jnp.float32)
    pressure = bell_draw(arg_keys[10], (NFX, NFY, NFZ), 1.0, 6.0, ((0, 4), (1, 4), (2, 2)), jnp.float32)
    pressure_source = bell_draw(arg_keys[11], (NFX, NFY, NFZ), 1.0, 6.0, ((0, 4), (1, 4), (2, 2)), jnp.float32)
    return {"positions": positions, "velocities": velocities, "spins": spins, "radii": radii, "counts": counts, "springs": springs, "partners": partners, "cells": cells, "departures": departures, "fluid_velocity": fluid_velocity, "pressure": pressure, "pressure_source": pressure_source}


normal_stiff = 100.0
normal_damp = 2.0
shear_stiff = 30.0
friction = 0.5
time_step = 0.05
drag_coeff = 0.8
gravity = 1.0
soft_length = 0.05
force_floor = 0.5
volume_coeff = 100.0
drag_weight = 1.0
neighbours = ((0, 0, 0), (-1, 0, 0), (1, 0, 0), (0, -1, 0), (0, 1, 0), (0, 0, -1), (0, 0, 1))
shift_table = ((0, -1, 1, 0, 0, 0, 0), (0, 0, 0, -1, 1, 0, 0), (0, 0, 0, 0, 0, -1, 1))

def row_normal(padded, row):
    slab = lax.dynamic_slice_in_dim(padded, row, 3, 1)
    extent_b = slab.shape[2] - 2
    extent_c = slab.shape[3] - 2
    centre = slab[:, 1, 1:1 + extent_b, 1:1 + extent_c]
    totals = [jnp.zeros_like(centre[0]) for axis_id in range(3)]
    for step_x, step_y, step_z in neighbours:
        other = slab[:, 1 + step_x, 1 + step_y:1 + step_y + extent_b, 1 + step_z:1 + step_z + extent_c]
        moves = (step_x, step_y, step_z)
        separation = [centre[axis_id][..., :, None] - other[axis_id][..., None, :] - float(moves[axis_id]) for axis_id in range(3)]
        distance = jnp.sqrt(separation[0] * separation[0] + separation[1] * separation[1] + separation[2] * separation[2] + soft_length ** 2)
        intersection = jnp.maximum(centre[9][..., :, None] + other[9][..., None, :] - distance, 0.0)
        root = jnp.sqrt(intersection)
        approach = sum(((centre[3 + axis_id][..., :, None] - other[3 + axis_id][..., None, :]) * separation[axis_id] for axis_id in range(3))) / distance
        weight = (normal_stiff * intersection * root - normal_damp * root * approach) * other[10][..., None, :] / distance
        totals = [totals[axis_id] + lax.optimization_barrier(jnp.sum(weight * separation[axis_id], axis=-1)) for axis_id in range(3)]
    return jnp.stack(totals)

def normal_forces(padded):
    rows = padded.shape[1] - 2
    stacked = lax.map(lambda row: row_normal(padded, row), jnp.arange(rows, dtype=jnp.int32))
    return jnp.moveaxis(stacked, 0, 1)

def partner_state(padded, codes):
    fields = padded.shape[0]
    extent_b = padded.shape[2]
    extent_c = padded.shape[3]
    slots = padded.shape[4]
    valid = (codes >= 0).astype(jnp.float32)
    code = jnp.maximum(codes, 0)
    which_bin = code // slots
    member = code % slots
    moves = []
    for axis_id in range(3):
        total = jnp.zeros_like(which_bin)
        for number in range(7):
            total = total + jnp.where(which_bin == number, shift_table[axis_id][number], 0).astype(jnp.int32)
        moves.append(total)
    index_a = lax.broadcasted_iota(jnp.int32, codes.shape, 1)
    index_b = lax.broadcasted_iota(jnp.int32, codes.shape, 2)
    index_c = lax.broadcasted_iota(jnp.int32, codes.shape, 3)
    linear = (((index_a + 1 + moves[0]) * extent_b + (index_b + 1 + moves[1])) * extent_c + (index_c + 1 + moves[2])) * slots + member
    flat = padded.reshape(fields, -1)
    picked = jnp.take(flat, linear.reshape(-1).astype(jnp.int32), axis=1).reshape((fields,) + codes.shape)
    return (picked, valid, [move.astype(jnp.float32) for move in moves])

def advance(padded, fluid_u, springs, codes):
    centre = padded[:, 1:-1, 1:-1, 1:-1]
    places = centre[0:3]
    speeds = centre[3:6]
    turning = centre[6:9]
    radius = centre[9]
    normal = normal_forces(padded)
    other, valid, moves = partner_state(padded, codes)
    separation = jnp.stack([places[axis_id][None] - other[axis_id] - moves[axis_id] for axis_id in range(3)])
    distance = jnp.sqrt(lax.optimization_barrier(jnp.sum(separation * separation, axis=0)) + soft_length ** 2)
    unit = separation / distance
    intersection = jnp.maximum(radius[None] + other[9] - distance, 0.0)
    root = jnp.sqrt(intersection)
    relative = speeds[:, None] - other[3:6]
    approach = lax.optimization_barrier(jnp.sum(relative * unit, axis=0))
    pressing = normal_stiff * intersection * root - normal_damp * root * approach
    lever = radius[None] * turning[:, None] + other[9] * other[6:9]
    contact = relative - jnp.cross(lever, unit, axis=0)
    sliding = contact - lax.optimization_barrier(jnp.sum(contact * unit, axis=0)) * unit
    stretched = springs - lax.optimization_barrier(jnp.sum(springs * unit, axis=0)) * unit + time_step * sliding
    length = jnp.sqrt(lax.optimization_barrier(jnp.sum(stretched * stretched, axis=0)))
    limit = jnp.minimum(1.0, friction * jnp.abs(pressing) / jnp.maximum(shear_stiff * length, force_floor))
    new_springs = valid * other[10] * limit * stretched
    shear = -shear_stiff * new_springs
    torque = radius * lax.optimization_barrier(jnp.sum(jnp.cross(shear, unit, axis=0), axis=1))
    safe = jnp.where(radius > 0.0, radius, 1.0)
    mass = (safe / 0.1) ** 3
    inertia = 0.4 * mass * safe * safe
    force = normal + lax.optimization_barrier(jnp.sum(shear, axis=1)) + drag_coeff * (fluid_u - speeds)
    lift = jnp.array([0.0, 0.0, gravity], dtype=jnp.float32).reshape(3, 1, 1, 1, 1)
    new_speeds = speeds + time_step * (force / mass - lift)
    new_turning = turning + time_step * torque / inertia
    new_places = places + time_step * new_speeds
    return (new_places, new_speeds, new_turning, new_springs)

def move_along(block, axis_id, step):
    extent = block.shape[axis_id]
    widths = [(0, 0)] * block.ndim
    if step == 1:
        widths[axis_id] = (1, 0)
        return lax.slice_in_dim(jnp.pad(block, widths), 0, extent, axis=axis_id)
    widths[axis_id] = (0, 1)
    return lax.slice_in_dim(jnp.pad(block, widths), 1, extent + 1, axis=axis_id)

def global_cells(cells):
    span_x = FX // BX
    span_y = FY // BY
    span_z = FZ // BZ
    off_z = cells % span_z
    off_y = cells // span_z % span_y
    off_x = cells // (span_z * span_y)
    corner_x = lax.broadcasted_iota(jnp.int32, cells.shape, 0) * span_x
    corner_y = lax.broadcasted_iota(jnp.int32, cells.shape, 1) * span_y
    corner_z = lax.broadcasted_iota(jnp.int32, cells.shape, 2) * span_z
    whole_x = corner_x + off_x
    whole_y = corner_y + off_y
    whole_z = corner_z + off_z
    return ((whole_x * NFY + whole_y) * NFZ + whole_z).astype(jnp.int32)

def reference(positions, velocities, spins, radii, counts, springs, partners, cells, departures, fluid_velocity, pressure, pressure_source):
    slot_index = lax.broadcasted_iota(jnp.int32, radii.shape, 3)
    live = (slot_index < counts[..., None]).astype(jnp.float32)
    whole_cells = global_cells(cells)
    fluid_u = jnp.take(fluid_velocity.reshape(3, -1), whole_cells.reshape(-1), axis=1).reshape((3,) + cells.shape)
    state = jnp.concatenate([positions, velocities, spins, radii[None], live[None]], 0)
    for step in range(SUBSTEPS):
        padded = jnp.pad(state, ((0, 0), (1, 1), (1, 1), (1, 1), (0, 0)))
        places, speeds, turning, springs = advance(padded, fluid_u, springs, partners)
        state = jnp.concatenate([places, speeds, turning, state[9:11]], 0)
    volume = 4.0 / 3.0 * math.pi * radii ** 3 * live
    values = jnp.concatenate([drag_coeff * (speeds - fluid_u) * live, volume[None]], 0).reshape(4, -1)
    sums = jnp.zeros((4, NFX * NFY * NFZ), jnp.float32).at[:, whole_cells.reshape(-1)].add(values)
    fluid_force = sums[0:3].reshape(3, NFX, NFY, NFZ)
    rhs = pressure_source + volume_coeff * sums[3].reshape(NFX, NFY, NFZ) + drag_weight * fluid_force[2]
    beside_all = jnp.pad(pressure, 1)
    neighbour_sum = beside_all[2:, 1:-1, 1:-1] + beside_all[:-2, 1:-1, 1:-1] + beside_all[1:-1, 2:, 1:-1] + beside_all[1:-1, :-2, 1:-1] + beside_all[1:-1, 1:-1, 2:] + beside_all[1:-1, 1:-1, :-2]
    new_pressure = (neighbour_sum + rhs) / 6.0
    lanes = departures.shape
    device_x = lax.broadcasted_iota(jnp.int32, lanes, 0)
    device_y = lax.broadcasted_iota(jnp.int32, lanes, 1)
    device_z = lax.broadcasted_iota(jnp.int32, lanes, 2)
    index = jnp.maximum(departures, 0)
    member = index % SLOTS
    remain = index // SLOTS
    bin_z = remain % BZ
    bin_y = remain // BZ % BY
    bin_x = remain // (BZ * BY)
    global_x = device_x * BX + bin_x
    global_y = device_y * BY + bin_y
    global_z = device_z * BZ + bin_z
    valid = (departures >= 0).astype(jnp.float32)
    carried = jnp.concatenate([places, speeds, turning, radii[None], springs.reshape((3 * HIST,) + radii.shape)], 0)
    taken = carried[:, global_x, global_y, global_z, member] * valid
    taken_codes = jnp.where(departures >= 0, partners[:, global_x, global_y, global_z, member] + 1, 0).astype(jnp.int32)
    taken = jnp.moveaxis(taken, 0, 3)
    taken_codes = jnp.moveaxis(taken_codes, 0, 3)
    got = []
    got_codes = []
    for direction in range(6):
        step = -1 if direction % 2 == 0 else 1
        got.append(move_along(taken[:, :, :, :, direction], direction // 2, step))
        got_codes.append(move_along(taken_codes[:, :, :, :, direction], direction // 2, step))
    arrived = jnp.stack(got, axis=4)
    arrived_partners = (jnp.stack(got_codes, axis=4) - 1).astype(jnp.int32)
    return (places, speeds, turning, springs, fluid_force, new_pressure, arrived, arrived_partners)
```

```python
import functools
import math

import jax
import jax.numpy as jnp
from jax import lax
from jax.experimental import pallas as pl
from jax.experimental.pallas import tpu as pltpu
from jax.sharding import PartitionSpec as P

SUBSTEPS = 2

normal_stiff = 100.0
normal_damp = 2.0
shear_stiff = 30.0
friction = 0.5
time_step = 0.05
drag_coeff = 0.8
gravity = 1.0
soft_length = 0.05
force_floor = 0.5
volume_coeff = 100.0
neighbours = ((0, 0, 0), (-1, 0, 0), (1, 0, 0), (0, -1, 0), (0, 1, 0), (0, 0, -1), (0, 0, 1))
AXES = ("gx", "gy", "gz")
FIELDS = 10
DEAD = -8.0
TINY = 1e-30
GROUP = 4
f32 = jnp.float32


class Plan:
    def __init__(self, shape):
        self.dims = shape
        self.count = shape[0] * shape[1] * shape[2]

    def index(self, place):
        return (place[0] * self.dims[1] + place[1]) * self.dims[2] + place[2]

    def places(self):
        d = self.dims
        return [(a, b, c) for a in range(d[0]) for b in range(d[1]) for c in range(d[2])]

    def face(self, axis, side):
        edge = self.dims[axis] - 1 if side > 0 else 0
        return [self.index(p) for p in self.places() if p[axis] == edge]

    def neighbour(self, place, number):
        move = neighbours[number]
        other = tuple(p + m for p, m in zip(place, move))
        if all(0 <= o < d for o, d in zip(other, self.dims)):
            return True, self.index(other)
        axis = (number - 1) // 2
        across = [o for k, o in enumerate(place) if k != axis]
        width = [d for k, d in enumerate(self.dims) if k != axis][1]
        return False, across[0] * width + across[1]


def rolls(axis, size):
    if axis == "gx" and size > 2:
        return [
            [(i, (i + 1) % size) for i in range(size)],
            [((i + 1) % size, i) for i in range(size)],
        ]
    out = []
    for start in range(2 if size > 2 else 1):
        pairs = []
        for i in range(start, size - 1, 2):
            pairs += [(i, i + 1), (i + 1, i)]
        out.append(pairs)
    return out


def is_ring(axis, size):
    return axis == "gx" and size > 2


def ordered_send(axis, size, low, high):
    if is_ring(axis, size):
        return [high, low]
    even = lax.axis_index(axis) % 2 == 0
    first = jnp.where(even, high, low)
    if size == 2:
        return [first]
    return [first, jnp.where(even, low, high)]


def ordered_receive(axis, size, blocks):
    if is_ring(axis, size):
        return blocks[0], blocks[1]
    if size == 2:
        return blocks[0], blocks[0]
    even = lax.axis_index(axis) % 2 == 0
    return jnp.where(even, blocks[1], blocks[0]), jnp.where(even, blocks[0], blocks[1])


def at_end(axis, size, side):
    edge = size - 1 if side > 0 else 0
    return lax.axis_index(axis) == edge


def exchange(blocks, sizes):
    out = []
    k = 0
    for axis, size in zip(AXES, sizes):
        for pairs in rolls(axis, size):
            out.append(lax.ppermute(blocks[k], axis, pairs))
            k += 1
    return out


def per_axis(refs, sizes):
    out = []
    k = 0
    for axis, size in zip(AXES, sizes):
        n = len(rolls(axis, size))
        out.append(refs[k : k + n])
        k += n
    return out


def send_count(sizes):
    return sum(len(rolls(a, s)) for a, s in zip(AXES, sizes))


def put_faces(plan, sizes, state_ref, send_refs):
    for axis, refs in enumerate(per_axis(send_refs, sizes)):
        low = plan.face(axis, -1)
        high = plan.face(axis, 1)
        width = len(low)
        for k in range(width):
            a = state_ref[:, low[k], :]
            b = state_ref[:, high[k], :]
            for ref, block in zip(refs, ordered_send(AXES[axis], sizes[axis], a, b)):
                ref[pl.ds(k, FIELDS, stride=width), :] = block


def pack_kernel(plan, sizes, pos, vel, spin, rad, counts, pressure, *outs):
    state = outs[0]
    sends = outs[1:]
    state[0:3] = pos[...]
    state[3:6] = vel[...]
    state[6:9] = spin[...]
    slots = rad.shape[-1]
    lane = lax.broadcasted_iota(jnp.int32, (1, slots), 1)
    for b in range(plan.count):
        state[9, b : b + 1, :] = jnp.where(lane < counts[b], rad[b : b + 1, :], DEAD)
    put_faces(plan, sizes, state, sends)
    nx, ny, nz = pressure.shape
    lanes = slots
    chunks = nz // lanes
    split = per_axis(sends, sizes)
    base = FIELDS * len(plan.face(0, 1))
    for ref, block in zip(
        split[0], ordered_send("gx", sizes[0], pressure[0], pressure[nx - 1])
    ):
        for c in range(chunks):
            ref[base + c * ny : base + (c + 1) * ny, :] = block[:, c * lanes : (c + 1) * lanes]
    base = FIELDS * len(plan.face(1, 1))
    for ref, block in zip(
        split[1], ordered_send("gy", sizes[1], pressure[:, 0, :], pressure[:, ny - 1, :])
    ):
        for c in range(chunks):
            ref[base + c * nx : base + (c + 1) * nx, :] = block[:, c * lanes : (c + 1) * lanes]
    base = FIELDS * len(plan.face(2, 1))
    wide = lax.broadcasted_iota(jnp.int32, (ny, lanes), 1)
    low = jnp.zeros((ny, lanes), f32)
    high = jnp.zeros((ny, lanes), f32)
    for x in range(nx):
        low = jnp.where(wide == x, jnp.broadcast_to(pressure[x, :, 0:1], (ny, lanes)), low)
        high = jnp.where(
            wide == x, jnp.broadcast_to(pressure[x, :, nz - 1 : nz], (ny, lanes)), high
        )
    for ref, block in zip(split[2], ordered_send("gz", sizes[2], low, high)):
        ref[base : base + ny, :] = block


def spread_own(b, state, radius, spread, columns):
    for f in range(3):
        columns[f : f + 1, :] = state[f, b : b + 1, :]
        columns[3 + f : 4 + f, :] = state[3 + f, b : b + 1, :] * (normal_damp / normal_stiff)
    columns[6:7, :] = radius[b : b + 1, :]
    columns[7:8, :] = radius[b : b + 1, :]
    slots = columns.shape[-1]
    turned = jnp.transpose(columns[...], (1, 0))
    for f in range(7):
        spread[f] = jnp.broadcast_to(turned[:, f : f + 1], (slots, slots))


def pair_forces(b, chosen, others, spread, parts, total, first):
    slots = spread.shape[-1]
    trips = slots // (8 * GROUP)

    def trip(g, carry):
        for t in range(GROUP):
            rows = pl.ds(pl.multiple_of((g * GROUP + t) * 8, 8), 8)
            mine = [spread[f, rows, :] for f in range(7)]
            sums = None
            for n in chosen:
                their = [jnp.broadcast_to(others[n, f, b : b + 1, :], (8, slots)) for f in range(7)]
                sep = [mine[k] - their[k] for k in range(3)]
                square = sep[0] * sep[0] + (sep[1] * sep[1] + (sep[2] * sep[2] + soft_length**2))
                inverse = lax.rsqrt(square)
                over = (mine[6] + their[6]) - square * inverse
                positive = jnp.maximum(over, 0.0)
                root = positive * lax.rsqrt(jnp.maximum(over, TINY))
                dot = (mine[3] - their[3]) * sep[0]
                dot = dot + (mine[4] - their[4]) * sep[1]
                dot = dot + (mine[5] - their[5]) * sep[2]
                weight = (positive - dot * inverse) * (root * inverse)
                new = [weight * sep[k] for k in range(3)]
                sums = new if sums is None else [s + w for s, w in zip(sums, new)]
            for k in range(3):
                parts[k, rows, :] = sums[k]
        return carry

    lax.fori_loop(0, trips, trip, 0)
    for k in range(3):
        row = jnp.sum(jnp.transpose(parts[k], (1, 0)), axis=0, keepdims=True) * normal_stiff
        total[k, b : b + 1, :] = row if first else total[k, b : b + 1, :] + row


def scale_rows(n, place, rows):
    move = neighbours[n]
    return rows


def own_pairs(plan, state, radius, total, others, spread, columns, parts):
    scale = normal_damp / normal_stiff
    places = plan.places()
    for n in range(7):
        for place in places:
            own, other = plan.neighbour(place, n)
            b = plan.index(place)
            if not own:
                continue
            for f in range(3):
                row = state[f, other : other + 1, :]
                if neighbours[n][f]:
                    row = row + float(neighbours[n][f])
                others[n, f, b : b + 1, :] = row
                others[n, 3 + f, b : b + 1, :] = state[3 + f, other : other + 1, :] * scale
            others[n, 6, b : b + 1, :] = state[9, other : other + 1, :]
    for place in places:
        b = plan.index(place)
        spread_own(b, state, radius, spread, columns)
        chosen = [n for n in range(7) if plan.neighbour(place, n)[0]]
        pair_forces(b, chosen, others, spread, parts, total, True)


def inner_kernel(plan, with_fluid, *refs):
    if with_fluid:
        state, radius, cells, fluid, total, gas, others, spread, columns, parts = refs
    else:
        state, radius, total, others, spread, columns, parts = refs
    own_pairs(plan, state, radius, total, others, spread, columns, parts)
    if not with_fluid:
        return
    slots = radius.shape[-1]
    span = [s // d for s, d in zip(fluid.shape[1:], plan.dims)]
    sub = lax.broadcasted_iota(jnp.int32, (8, slots), 0)
    for place in plan.places():
        b = plan.index(place)
        cell = cells[b : b + 1, :]
        column = jnp.broadcast_to(cell % span[2], (8, slots))
        row = jnp.broadcast_to(cell // span[2], (8, slots)) - sub
        sums = [jnp.zeros((8, slots), f32) for c in range(3)]
        for a in range(span[0]):
            for h in range(span[1] // 8):
                hit = row == a * span[1] + h * 8
                y0 = place[1] * span[1] + h * 8
                z0 = place[2] * span[2]
                for c in range(3):
                    block = fluid[c, place[0] * span[0] + a, y0 : y0 + 8, z0 : z0 + span[2]]
                    got = jnp.take_along_axis(block, column, axis=1)
                    sums[c] = jnp.where(hit, got, sums[c])
        for c in range(3):
            gas[c, b : b + 1, :] = jnp.sum(sums[c], axis=0, keepdims=True)


def step_core(plan, sizes, state, radius, inner, springs, partners, gas, halos, out, new_springs,
              around, others, spread, columns, parts, outer):
    scale = normal_damp / normal_stiff
    places = plan.places()
    slots = radius.shape[-1]
    split = per_axis(halos, sizes)
    around[0] = state[...]
    for axis in range(3):
        width = len(plan.face(axis, 1))
        for place in places:
            b = plan.index(place)
            for side in (0, 1):
                n = 1 + 2 * axis + side
                own, other = plan.neighbour(place, n)
                if own:
                    around[n, :, b, :] = state[:, other, :]
                    continue
                got = [ref[pl.ds(other, FIELDS, stride=width), :] for ref in split[axis]]
                before, after = ordered_receive(AXES[axis], sizes[axis], got)
                around[n, :, b, :] = after if side else before
    sub = lax.broadcasted_iota(jnp.int32, (plan.count, slots), 0)
    inner_count = [plan.dims[1] * plan.dims[2], plan.dims[2], 1]
    for n in range(1, 7):
        axis = (n - 1) // 2
        side = 1 if n % 2 == 0 else -1
        edge = plan.dims[axis] - 1 if side > 0 else 0
        level = sub // inner_count[axis] % plan.dims[axis]
        outside = (level == edge) & at_end(AXES[axis], sizes[axis], side)
        reach = around[n, 9]
        around[n, 9] = jnp.where(outside | (reach <= 0.0), DEAD, reach)
        for f in range(3):
            others[n, f] = around[n, f] + float(neighbours[n][f])
            others[n, 3 + f] = around[n, 3 + f] * scale
        others[n, 6] = around[n, 9]
    for place in places:
        b = plan.index(place)
        chosen = [n for n in range(7) if not plan.neighbour(place, n)[0]]
        spread_own(b, state, radius, spread, columns)
        pair_forces(b, chosen, others, spread, parts, outer, True)
    place_i = [state[k] for k in range(3)]
    speed_i = [state[3 + k] for k in range(3)]
    turn_i = [state[6 + k] for k in range(3)]
    rad_i = radius[...]
    shear_sum = [jnp.zeros_like(rad_i) for k in range(3)]
    twist = [jnp.zeros_like(rad_i) for k in range(3)]
    for h in range(partners.shape[0]):
        code = partners[h]
        valid = code >= 0
        code = jnp.maximum(code, 0)
        which = code // slots
        member = code % slots
        picked = []
        for f in range(FIELDS):
            value = jnp.take_along_axis(around[0, f], member, axis=1)
            for n in range(1, 7):
                got = jnp.take_along_axis(around[n, f], member, axis=1)
                value = jnp.where(which == n, got, value)
            picked.append(value)
        alive = valid & (picked[9] > 0.0)
        sep = []
        for k in range(3):
            shift = jnp.where(which == 2 + 2 * k, 1.0, jnp.where(which == 1 + 2 * k, -1.0, 0.0))
            sep.append(place_i[k] - picked[k] - shift)
        distance = jnp.sqrt(sep[0] * sep[0] + sep[1] * sep[1] + sep[2] * sep[2] + soft_length**2)
        unit = [s / distance for s in sep]
        over = jnp.maximum(rad_i + picked[9] - distance, 0.0)
        root = jnp.sqrt(over)
        rel = [speed_i[k] - picked[3 + k] for k in range(3)]
        approach = rel[0] * unit[0] + rel[1] * unit[1] + rel[2] * unit[2]
        pressing = normal_stiff * over * root - normal_damp * root * approach
        lever = [rad_i * turn_i[k] + picked[9] * picked[6 + k] for k in range(3)]
        contact = [
            rel[k]
            - (
                lever[(k + 1) % 3] * unit[(k + 2) % 3]
                - lever[(k + 2) % 3] * unit[(k + 1) % 3]
            )
            for k in range(3)
        ]
        along = contact[0] * unit[0] + contact[1] * unit[1] + contact[2] * unit[2]
        old = [springs[k, h] for k in range(3)]
        old_along = old[0] * unit[0] + old[1] * unit[1] + old[2] * unit[2]
        stretched = [
            old[k] - old_along * unit[k] + time_step * (contact[k] - along * unit[k])
            for k in range(3)
        ]
        length = jnp.sqrt(
            stretched[0] * stretched[0] + stretched[1] * stretched[1] + stretched[2] * stretched[2]
        )
        limit = jnp.minimum(
            1.0, friction * jnp.abs(pressing) / jnp.maximum(shear_stiff * length, force_floor)
        )
        limit = jnp.where(alive, limit, 0.0)
        fresh = [limit * stretched[k] for k in range(3)]
        for k in range(3):
            new_springs[k, h] = fresh[k]
            shear_sum[k] = shear_sum[k] - shear_stiff * fresh[k]
            twist[k] = twist[k] - shear_stiff * (
                fresh[(k + 1) % 3] * unit[(k + 2) % 3] - fresh[(k + 2) % 3] * unit[(k + 1) % 3]
            )
    safe = jnp.where(rad_i > 0.0, rad_i, 1.0)
    ratio = safe / 0.1
    mass = ratio * ratio * ratio
    inertia = 0.4 * mass * safe * safe
    for k in range(3):
        force = inner[k] + outer[k] + shear_sum[k] + drag_coeff * (gas[k] - speed_i[k])
        lift = gravity if k == 2 else 0.0
        speed = speed_i[k] + time_step * (force / mass - lift)
        out[k] = place_i[k] + time_step * speed
        out[3 + k] = speed
        out[6 + k] = turn_i[k] + time_step * (rad_i * twist[k]) / inertia
    out[9] = state[9]


def middle_kernel(plan, sizes, *refs):
    n = send_count(sizes)
    state, radius, inner, springs, partners, gas = refs[:6]
    halos = refs[6 : 6 + n]
    out, new_springs = refs[6 + n : 8 + n]
    sends = refs[8 + n : 8 + 2 * n]
    scratch = refs[8 + 2 * n :]
    step_core(plan, sizes, state, radius, inner, springs, partners, gas, halos, out, new_springs,
              *scratch)
    put_faces(plan, sizes, out, sends)


def last_kernel(plan, sizes, *refs):
    n = send_count(sizes)
    state, radius, inner, springs, partners, gas, departures = refs[:7]
    halos = refs[7 : 7 + n]
    places, speeds, turns, new_springs = refs[7 + n : 11 + n]
    sends = refs[11 + n : 11 + 2 * n]
    out = refs[11 + 2 * n]
    scratch = refs[12 + 2 * n :]
    step_core(plan, sizes, state, radius, inner, springs, partners, gas, halos, out, new_springs,
              *scratch)
    places[...] = out[0:3]
    speeds[...] = out[3:6]
    turns[...] = out[6:9]
    slots = radius.shape[-1]
    hist = partners.shape[0]
    count = plan.count
    sub = lax.broadcasted_iota(jnp.int32, (count, slots), 0)
    values = [out[f] for f in range(9)] + [radius[...]]
    values += [new_springs[k, h] for k in range(3) for h in range(hist)]
    values += [(partners[h] + 1).astype(f32) for h in range(hist)]
    width = len(values)
    picks = [[], [], [], [], [], []]
    for d in range(6):
        leaving = jnp.broadcast_to(departures[d : d + 1, :], (count, slots))
        hit = (leaving // slots == sub) & (leaving >= 0)
        member = jnp.maximum(leaving, 0) % slots
        for v in values:
            got = jnp.where(hit, jnp.take_along_axis(v, member, axis=1), 0.0)
            picks[d].append(jnp.sum(got, axis=0, keepdims=True))
    split = per_axis(sends, sizes)
    for axis in range(3):
        for f in range(width):
            blocks = ordered_send(
                AXES[axis], sizes[axis], picks[2 * axis][f], picks[2 * axis + 1][f]
            )
            for ref, block in zip(split[axis], blocks):
                ref[f : f + 1, :] = block


def deposit_kernel(plan, sizes, *refs):
    n = send_count(sizes)
    state, radius, counts, cells, gas, pressure, source = refs[:7]
    halos = refs[7 : 7 + n]
    force, new_pressure = refs[7 + n :]
    slots = radius.shape[-1]
    nx, ny, nz = pressure.shape
    lanes = slots
    chunks = nz // lanes
    span = [s // d for s, d in zip(pressure.shape, plan.dims)]
    rows = span[0] * span[1]
    lane = lax.broadcasted_iota(jnp.int32, (1, slots), 1)
    high_row = lax.broadcasted_iota(jnp.int32, (rows, slots), 0)
    column_row = lax.broadcasted_iota(jnp.int32, (span[2], slots), 0)
    for place in plan.places():
        b = plan.index(place)
        cell = cells[b : b + 1, :]
        live = lane < counts[b]
        rad = radius[b : b + 1, :]
        values = [
            jnp.where(live, drag_coeff * (state[c, b : b + 1, :] - gas[c, b : b + 1, :]), 0.0)
            for c in range(3)
        ]
        values.append(jnp.where(live, 4.0 / 3.0 * math.pi * rad * rad * rad, 0.0))
        at_row = high_row == cell // span[2]
        at_column = (column_row == cell % span[2]).astype(jnp.bfloat16)
        halves = []
        for v in values:
            top = v.astype(jnp.bfloat16).astype(f32)
            left = v - top
            mid = left.astype(jnp.bfloat16).astype(f32)
            low = left - mid
            halves.append(
                jnp.concatenate(
                    [jnp.where(at_row, part, 0.0).astype(jnp.bfloat16) for part in (top, mid, low)],
                    axis=1,
                )
            )
        left = jnp.concatenate(halves, axis=0)
        right = jnp.concatenate([at_column] * 3, axis=1)
        got = lax.dot_general(
            left, right, (((1,), (1,)), ((), ())), preferred_element_type=f32
        )
        x0, y0, z0 = (p * s for p, s in zip(place, span))
        block = (slice(x0, x0 + span[0]), slice(y0, y0 + span[1]), slice(z0, z0 + span[2]))
        pieces = [got[c * rows : (c + 1) * rows].reshape(span) for c in range(4)]
        for c in range(3):
            force[(c,) + block] = pieces[c]
        new_pressure[block] = volume_coeff * pieces[3] + pieces[2]
    split = per_axis(halos, sizes)
    dead = [
        [at_end(AXES[axis], sizes[axis], side) for side in (-1, 1)] for axis in range(3)
    ]
    base = FIELDS * len(plan.face(0, 1))
    slabs = []
    for ref in split[0]:
        slabs.append(
            jnp.concatenate(
                [ref[base + c * ny : base + (c + 1) * ny, :] for c in range(chunks)], axis=1
            )
        )
    x_ends = ordered_receive("gx", sizes[0], slabs)
    x_ends = [jnp.where(dead[0][s], 0.0, x_ends[s]) for s in (0, 1)]
    base = FIELDS * len(plan.face(1, 1))
    slabs = []
    for ref in split[1]:
        slabs.append(
            jnp.concatenate(
                [ref[base + c * nx : base + (c + 1) * nx, :] for c in range(chunks)], axis=1
            )
        )
    y_ends = ordered_receive("gy", sizes[1], slabs)
    y_ends = [jnp.where(dead[1][s], 0.0, y_ends[s]) for s in (0, 1)]
    base = FIELDS * len(plan.face(2, 1))
    z_ends = ordered_receive("gz", sizes[2], [ref[base : base + ny, :] for ref in split[2]])
    z_ends = [jnp.where(dead[2][s], 0.0, z_ends[s]) for s in (0, 1)]
    row = lax.broadcasted_iota(jnp.int32, (ny, nz), 0)
    column = lax.broadcasted_iota(jnp.int32, (ny, nz), 1)
    for x in range(nx):
        here = pressure[x]
        total = pressure[x - 1] if x > 0 else x_ends[0]
        total = total + (pressure[x + 1] if x < nx - 1 else x_ends[1])
        total = total + jnp.where(row == 0, y_ends[0][x : x + 1, :], pltpu.roll(here, 1, 0))
        total = total + jnp.where(
            row == ny - 1, y_ends[1][x : x + 1, :], pltpu.roll(here, ny - 1, 0)
        )
        total = total + jnp.where(column == 0, z_ends[0][:, x : x + 1], pltpu.roll(here, 1, 1))
        total = total + jnp.where(
            column == nz - 1, z_ends[1][:, x : x + 1], pltpu.roll(here, nz - 1, 1)
        )
        new_pressure[x] = (total + (source[x] + new_pressure[x])) * (1.0 / 6.0)


def arrive_kernel(sizes, *refs):
    n = send_count(sizes)
    halos = refs[:n]
    state, codes = refs[n:]
    split = per_axis(halos, sizes)
    width = state.shape[0]
    hist = codes.shape[0]
    for axis in range(3):
        got = [ref[0 : width + hist, :] for ref in split[axis]]
        before, after = ordered_receive(AXES[axis], sizes[axis], got)
        after = jnp.where(at_end(AXES[axis], sizes[axis], 1), 0.0, after)
        before = jnp.where(at_end(AXES[axis], sizes[axis], -1), 0.0, before)
        for d, block in ((2 * axis, after), (2 * axis + 1, before)):
            state[:, d, :] = block[0:width]
            codes[:, d, :] = block[width : width + hist].astype(jnp.int32) - 1


def call(kernel, outs, scratch, args, smem=(), flops=0):
    specs = [
        pl.BlockSpec(memory_space=pltpu.SMEM) if k in smem else pl.BlockSpec(memory_space=pltpu.VMEM)
        for k in range(len(args))
    ]
    return pl.pallas_call(
        kernel,
        out_shape=[jax.ShapeDtypeStruct(s, d) for s, d in outs],
        in_specs=specs,
        out_specs=[pl.BlockSpec(memory_space=pltpu.VMEM)] * len(outs),
        scratch_shapes=scratch,
        compiler_params=pltpu.CompilerParams(vmem_limit_bytes=32 * 1024 * 1024),
        cost_estimate=pl.CostEstimate(flops=flops, bytes_accessed=1 << 20, transcendentals=0),
    )(*args)


def body(sizes, positions, velocities, spins, radii, counts, springs, partners, cells, departures,
         fluid_velocity, pressure, pressure_source):
    plan = Plan(radii.shape[:3])
    count = plan.count
    slots = radii.shape[3]
    hist = partners.shape[0]
    nx, ny, nz = pressure.shape
    chunks = nz // slots
    flat = lambda a: a.reshape(a.shape[:-4] + (count, slots))
    pos, vel, spin = flat(positions), flat(velocities), flat(spins)
    radius = radii.reshape(count, slots)
    springs = springs.reshape(3, hist, count, slots)
    partners = partners.reshape(hist, count, slots)
    cells = cells.reshape(count, slots)
    counts = counts.reshape(count)
    leaving = departures.reshape(6, slots)

    faces = [FIELDS * len(plan.face(a, 1)) for a in range(3)]
    extra = [chunks * ny, chunks * nx, ny]
    vm = lambda *s: pltpu.VMEM(s, f32)

    def sends(rows):
        out = []
        for a in range(3):
            for _ in rolls(AXES[a], sizes[a]):
                out.append(((rows[a], slots), f32))
        return out

    pair_scratch = [vm(7, 7, count, slots), vm(7, slots, slots), vm(8, slots), vm(3, slots, slots)]
    step_scratch = [vm(7, FIELDS, count, slots)] + pair_scratch + [vm(3, count, slots)]
    state_shape = ((FIELDS, count, slots), f32)
    three = ((3, count, slots), f32)
    spring_shape = ((3, hist, count, slots), f32)
    bind = functools.partial

    state, *out = call(
        bind(pack_kernel, plan, sizes),
        [state_shape] + sends([f + e for f, e in zip(faces, extra)]),
        [],
        [pos, vel, spin, radius, counts, pressure],
        smem=(4,),
        flops=1 << 20,
    )
    first_halos = exchange(out, sizes)
    inner, gas = call(
        bind(inner_kernel, plan, True),
        [three, three],
        pair_scratch,
        [state, radius, cells, fluid_velocity],
        flops=1 << 25,
    )
    state, springs, *out = call(
        bind(middle_kernel, plan, sizes),
        [state_shape, spring_shape] + sends(faces),
        step_scratch,
        [state, radius, inner, springs, partners, gas] + first_halos,
        flops=1 << 25,
    )
    halos = exchange(out, sizes)
    (inner,) = call(
        bind(inner_kernel, plan, False), [three], pair_scratch, [state, radius], flops=1 << 25
    )
    width = 10 + 4 * hist
    padded = (width + 7) // 8 * 8
    places, speeds, turns, springs, *out = call(
        bind(last_kernel, plan, sizes),
        [three, three, three, spring_shape] + sends([padded] * 3),
        [vm(FIELDS, count, slots)] + step_scratch,
        [state, radius, inner, springs, partners, gas, leaving] + halos,
        flops=1 << 25,
    )
    arrivals = exchange(out, sizes)
    force, new_pressure = call(
        bind(deposit_kernel, plan, sizes),
        [((3, nx, ny, nz), f32), ((nx, ny, nz), f32)],
        [],
        [speeds, radius, counts, cells, gas, pressure, pressure_source] + first_halos,
        smem=(2,),
        flops=1 << 25,
    )
    arrived, arrived_partners = call(
        bind(arrive_kernel, sizes),
        [((10 + 3 * hist, 6, slots), f32), ((hist, 6, slots), jnp.int32)],
        [],
        arrivals,
        flops=1 << 20,
    )
    wide = lambda a: a.reshape(a.shape[:-2] + radii.shape)
    return (
        wide(places),
        wide(speeds),
        wide(turns),
        wide(springs),
        force,
        new_pressure,
        arrived[None, None, None],
        arrived_partners[None, None, None],
    )


def solution(mesh):
    sizes = tuple(mesh.shape[a] for a in AXES)
    return jax.shard_map(
        functools.partial(body, sizes),
        mesh=mesh,
        in_specs=(
            P(None, "gx", "gy", "gz", None),
            P(None, "gx", "gy", "gz", None),
            P(None, "gx", "gy", "gz", None),
            P("gx", "gy", "gz", None),
            P("gx", "gy", "gz"),
            P(None, None, "gx", "gy", "gz", None),
            P(None, "gx", "gy", "gz", None),
            P("gx", "gy", "gz", None),
            P("gx", "gy", "gz", None, None),
            P(None, "gx", "gy", "gz"),
            P("gx", "gy", "gz"),
            P("gx", "gy", "gz"),
        ),
        out_specs=(
            P(None, "gx", "gy", "gz", None),
            P(None, "gx", "gy", "gz", None),
            P(None, "gx", "gy", "gz", None),
            P(None, None, "gx", "gy", "gz", None),
            P(None, "gx", "gy", "gz"),
            P("gx", "gy", "gz"),
            P("gx", "gy", "gz", None, None, None),
            P("gx", "gy", "gz", None, None, None),
        ),
        check_vma=False,
    )
```

```python
import functools
import math

import jax
import jax.numpy as jnp
from jax import lax
from jax.experimental import pallas as pl
from jax.experimental.pallas import tpu as pltpu
from jax.sharding import PartitionSpec as P

SUBSTEPS = 2

normal_stiff = 100.0
normal_damp = 2.0
shear_stiff = 30.0
friction = 0.5
time_step = 0.05
drag_coeff = 0.8
gravity = 1.0
soft_length = 0.05
force_floor = 0.5
volume_coeff = 100.0
neighbours = ((0, 0, 0), (-1, 0, 0), (1, 0, 0), (0, -1, 0), (0, 1, 0), (0, 0, -1), (0, 0, 1))
AXES = ("gx", "gy", "gz")
FIELDS = 10
DEAD = -8.0
TINY = 1e-30
f32 = jnp.float32


class Plan:
    def __init__(self, shape):
        self.dims = shape
        self.count = shape[0] * shape[1] * shape[2]

    def index(self, place):
        return (place[0] * self.dims[1] + place[1]) * self.dims[2] + place[2]

    def places(self):
        d = self.dims
        return [(a, b, c) for a in range(d[0]) for b in range(d[1]) for c in range(d[2])]

    def face(self, axis, side):
        edge = self.dims[axis] - 1 if side > 0 else 0
        return [self.index(p) for p in self.places() if p[axis] == edge]

    def neighbour(self, place, number):
        move = neighbours[number]
        other = tuple(p + m for p, m in zip(place, move))
        if all(0 <= o < d for o, d in zip(other, self.dims)):
            return True, self.index(other)
        axis = (number - 1) // 2
        across = [o for k, o in enumerate(place) if k != axis]
        width = [d for k, d in enumerate(self.dims) if k != axis][1]
        return False, across[0] * width + across[1]


def rolls(axis, sizes):
    size = sizes[AXES.index(axis)]
    if is_ring(axis, size):
        return [
            (axis, [(i, (i + 1) % size) for i in range(size)]),
            (axis, [((i + 1) % size, i) for i in range(size)]),
        ]

    def swaps(start):
        pairs = []
        for i in range(start, size - 1, 2):
            pairs += [(i, i + 1), (i + 1, i)]
        return pairs

    out = [(axis, swaps(0))]
    if size > 2:
        pairs = swaps(1)
        inside = [i for i, _ in pairs]
        across = sizes[0]
        if axis != "gx" and across % 2 == 0:
            joint = []
            for x in range(across):
                joint += [(x * size + i, x * size + j) for i, j in pairs]
                joint += [(x * size + i, (x ^ 1) * size + i) for i in range(size) if i not in inside]
            out.append((("gx", axis), joint))
        else:
            out.append((axis, pairs))
    return out


def is_ring(axis, size):
    return axis == "gx" and size > 2


def ordered_send(axis, size, low, high):
    if is_ring(axis, size):
        return [high, low]
    even = lax.axis_index(axis) % 2 == 0
    first = jnp.where(even, high, low)
    if size == 2:
        return [first]
    return [first, jnp.where(even, low, high)]


def ordered_receive(axis, size, blocks):
    if is_ring(axis, size):
        return blocks[0], blocks[1]
    if size == 2:
        return blocks[0], blocks[0]
    even = lax.axis_index(axis) % 2 == 0
    return jnp.where(even, blocks[1], blocks[0]), jnp.where(even, blocks[0], blocks[1])


def at_end(axis, size, side):
    edge = size - 1 if side > 0 else 0
    return lax.axis_index(axis) == edge


def exchange(blocks, sizes):
    routes = [route for axis in AXES for route in rolls(axis, sizes)]
    return [lax.ppermute(block, axes, pairs) for block, (axes, pairs) in zip(blocks, routes)]


def per_axis(refs, sizes):
    out = []
    k = 0
    for axis in AXES:
        n = len(rolls(axis, sizes))
        out.append(refs[k : k + n])
        k += n
    return out


def send_count(sizes):
    return sum(len(rolls(a, sizes)) for a in AXES)


def put_faces(plan, sizes, state_ref, send_refs):
    for axis, refs in enumerate(per_axis(send_refs, sizes)):
        low = plan.face(axis, -1)
        high = plan.face(axis, 1)
        width = len(low)
        for k in range(width):
            a = state_ref[:, low[k], :]
            b = state_ref[:, high[k], :]
            for ref, block in zip(refs, ordered_send(AXES[axis], sizes[axis], a, b)):
                ref[pl.ds(k, FIELDS, stride=width), :] = block


def pack_kernel(plan, sizes, pos, vel, spin, rad, counts_hbm, pressure_hbm, *refs):
    state, radius = refs[:2]
    sends = refs[2:-3]
    counts, pressure, sems = refs[-3:]
    copies = [
        pltpu.make_async_copy(rad, radius, sems.at[0]),
        pltpu.make_async_copy(pos, state.at[0:3], sems.at[1]),
        pltpu.make_async_copy(vel, state.at[3:6], sems.at[2]),
        pltpu.make_async_copy(spin, state.at[6:9], sems.at[3]),
        pltpu.make_async_copy(counts_hbm, counts, sems.at[4]),
        pltpu.make_async_copy(pressure_hbm, pressure, sems.at[5]),
    ]
    for copy in copies:
        copy.start()
    slots = rad.shape[-1]
    lane = lax.broadcasted_iota(jnp.int32, (1, slots), 1)
    places = plan.places()
    for copy in copies[:5]:
        copy.wait()
    for b in range(plan.count):
        x, y, z = places[b]
        live = lane < counts[x, y : y + 1, z : z + 1]
        state[9, b : b + 1, :] = jnp.where(live, radius[b : b + 1, :], DEAD)
    put_faces(plan, sizes, state, sends)
    copies[5].wait()
    nx, ny, nz = pressure.shape
    lanes = slots
    chunks = nz // lanes
    split = per_axis(sends, sizes)
    base = FIELDS * len(plan.face(0, 1))
    for ref, block in zip(
        split[0], ordered_send("gx", sizes[0], pressure[0], pressure[nx - 1])
    ):
        for c in range(chunks):
            ref[base + c * ny : base + (c + 1) * ny, :] = block[:, c * lanes : (c + 1) * lanes]
    base = FIELDS * len(plan.face(1, 1))
    for ref, block in zip(
        split[1], ordered_send("gy", sizes[1], pressure[:, 0, :], pressure[:, ny - 1, :])
    ):
        for c in range(chunks):
            ref[base + c * nx : base + (c + 1) * nx, :] = block[:, c * lanes : (c + 1) * lanes]
    base = FIELDS * len(plan.face(2, 1))
    wide = lax.broadcasted_iota(jnp.int32, (ny, lanes), 1)
    low = jnp.zeros((ny, lanes), f32)
    high = jnp.zeros((ny, lanes), f32)
    for x in range(nx):
        low = jnp.where(wide == x, jnp.broadcast_to(pressure[x, :, 0:1], (ny, lanes)), low)
        high = jnp.where(
            wide == x, jnp.broadcast_to(pressure[x, :, nz - 1 : nz], (ny, lanes)), high
        )
    for ref, block in zip(split[2], ordered_send("gz", sizes[2], low, high)):
        ref[base : base + ny, :] = block


def pair_rows(state, radius, mine):
    scale = normal_damp / normal_stiff
    for k in range(3):
        mine[:, k, :] = state[k]
        mine[:, 3 + k, :] = state[3 + k] * scale
    mine[:, 6, :] = radius[...]
    mine[:, 7, :] = radius[...]


def spread_rows(mine, spread):
    slots = mine.shape[-1]
    turned = [jnp.transpose(mine[b], (1, 0)) for b in range(mine.shape[0])]
    for b in range(mine.shape[0]):
        for f in range(7):
            spread[b, f] = jnp.broadcast_to(turned[b][:, f : f + 1], (slots, slots))


def list_pairs(plan, entries, packed, table):
    slots = packed.shape[-1]
    lane = lax.broadcasted_iota(jnp.int32, (8, slots), 1)
    field = lax.broadcasted_iota(jnp.int32, (8, slots), 0)
    empty = jnp.where(field == 6, DEAD, 0.0)
    jobs = jnp.int32(0)
    for b in range(plan.count):
        start = jobs
        at = None
        for rows, count, move in entries[b]:
            value = rows
            for k in range(3):
                if move[k]:
                    value = value + jnp.where(field == k, float(move[k]), 0.0)
            if at is None:
                packed[start] = jnp.where(lane < count, value, empty)
                packed[start + 1] = empty
                at = count
                continue
            shift = at % slots
            job = start + at // slots
            moved = pltpu.roll(value, shift, 1)
            packed[job] = jnp.where(
                (lane >= shift) & (lane < shift + count), moved, packed[job]
            )
            packed[job + 1] = jnp.where(lane < shift + count - slots, moved, empty)
            at = at + count
        jobs = start + (at + slots - 1) // slots
        for q in range(len(entries[b])):
            table[start + q] = b
    return jobs


def run_pairs(jobs, spread, packed, table, parts):
    slots = packed.shape[-1]

    def job(t, carry):
        b = table[t]
        their = [jnp.broadcast_to(packed[t, f : f + 1, :], (8, slots)) for f in range(7)]
        for tile in range(slots // 8):
            rows = slice(tile * 8, tile * 8 + 8)
            own = [spread[b, f, rows, :] for f in range(7)]
            sep = [own[k] - their[k] for k in range(3)]
            square = sep[0] * sep[0] + (sep[1] * sep[1] + (sep[2] * sep[2] + soft_length**2))
            inverse = lax.rsqrt(square)
            over = (own[6] + their[6]) - square * inverse
            positive = jnp.maximum(over, 0.0)
            root = positive * lax.rsqrt(jnp.maximum(over, TINY))
            dot = (own[3] - their[3]) * sep[0]
            dot = dot + (own[4] - their[4]) * sep[1]
            dot = dot + (own[5] - their[5]) * sep[2]
            weight = (positive - dot * inverse) * (root * inverse)
            for k in range(3):
                parts[b, k, rows, :] = parts[b, k, rows, :] + weight * sep[k]
        return carry

    lax.fori_loop(0, jobs, job, 0)


def inner_kernel(plan, with_fluid, *refs):
    if with_fluid:
        (state, radius, cells_hbm, fluid_hbm, spread, parts, gas, cells, mine, packed,
         table, fluid, sems) = refs
        fetches = [
            pltpu.make_async_copy(cells_hbm, cells, sems.at[0]),
            pltpu.make_async_copy(fluid_hbm, fluid, sems.at[1]),
        ]
        for fetch in fetches:
            fetch.start()
    else:
        state, radius, spread, parts, mine, packed, table = refs
    parts[...] = jnp.zeros_like(parts)
    pair_rows(state, radius, mine)
    spread_rows(mine, spread)
    records = []
    for b in range(plan.count):
        rows = mine[b]
        field = lax.broadcasted_iota(jnp.int32, rows.shape, 0)
        records.append(jnp.where(field == 6, state[9, b : b + 1, :], rows))
    filled = jnp.sum(jnp.where(state[9] > 0.0, 1, 0), axis=1, keepdims=True)
    entries = []
    for place in plan.places():
        entry = []
        for n in range(7):
            own, other = plan.neighbour(place, n)
            if own:
                entry.append((records[other], filled[other, 0], neighbours[n]))
        entries.append(entry)
    jobs = list_pairs(plan, entries, packed, table)
    run_pairs(jobs, spread, packed, table, parts)
    if not with_fluid:
        return
    for fetch in fetches:
        fetch.wait()
    slots = radius.shape[-1]
    span = [s // d for s, d in zip(fluid.shape[1:], plan.dims)]
    sub = lax.broadcasted_iota(jnp.int32, (8, slots), 0)
    for place in plan.places():
        b = plan.index(place)
        cell = cells[b : b + 1, :]
        column = jnp.broadcast_to(cell % span[2], (8, slots))
        row = jnp.broadcast_to(cell // span[2], (8, slots)) - sub
        sums_c = [jnp.zeros((8, slots), f32) for c in range(3)]
        for a in range(span[0]):
            for h in range(span[1] // 8):
                hit = row == a * span[1] + h * 8
                y0 = place[1] * span[1] + h * 8
                z0 = place[2] * span[2]
                for c in range(3):
                    block = fluid[c, place[0] * span[0] + a, y0 : y0 + 8, z0 : z0 + span[2]]
                    got = jnp.take_along_axis(block, column, axis=1)
                    sums_c[c] = jnp.where(hit, got, sums_c[c])
        for c in range(3):
            gas[c, b : b + 1, :] = jnp.sum(sums_c[c], axis=0, keepdims=True)


def step_core(plan, sizes, state, radius, spread, inner, springs, partners, gas, halos, out,
              new_springs, around, packed, table, parts):
    scale = normal_damp / normal_stiff
    places = plan.places()
    slots = radius.shape[-1]
    split = per_axis(halos, sizes)
    around[0] = state[...]
    for axis in range(3):
        width = len(plan.face(axis, 1))
        for place in places:
            b = plan.index(place)
            for side in (0, 1):
                n = 1 + 2 * axis + side
                own, other = plan.neighbour(place, n)
                if own:
                    around[n, :, b, :] = state[:, other, :]
                    continue
                got = [ref[pl.ds(other, FIELDS, stride=width), :] for ref in split[axis]]
                before, after = ordered_receive(AXES[axis], sizes[axis], got)
                around[n, :, b, :] = after if side else before
    sub = lax.broadcasted_iota(jnp.int32, (plan.count, slots), 0)
    inner_count = [plan.dims[1] * plan.dims[2], plan.dims[2], 1]
    entries = [[] for _ in places]
    parts[...] = inner[...]
    for n in range(1, 7):
        axis = (n - 1) // 2
        side = 1 if n % 2 == 0 else -1
        edge = plan.dims[axis] - 1 if side > 0 else 0
        level = sub // inner_count[axis] % plan.dims[axis]
        gone = at_end(AXES[axis], sizes[axis], side)
        reach = around[n, 9]
        reach = jnp.where(((level == edge) & gone) | (reach <= 0.0), DEAD, reach)
        around[n, 9] = reach
        filled = jnp.sum(jnp.where(reach > 0.0, 1, 0), axis=1, keepdims=True)
        for place in places:
            b = plan.index(place)
            if plan.neighbour(place, n)[0]:
                continue
            rows = around[n, 0:8, b, :]
            field = lax.broadcasted_iota(jnp.int32, rows.shape, 0)
            rows = jnp.where((field > 2) & (field < 6), rows * scale, rows)
            rows = jnp.where(field == 6, reach[b : b + 1, :], rows)
            entries[b].append((rows, filled[b, 0], neighbours[n]))
    jobs = list_pairs(plan, entries, packed, table)
    run_pairs(jobs, spread, packed, table, parts)
    normal = []
    for k in range(3):
        sums = [
            jnp.sum(jnp.transpose(parts[b, k], (1, 0)), axis=0, keepdims=True)
            for b in range(plan.count)
        ]
        normal.append(jnp.concatenate(sums, axis=0) * normal_stiff)
    place_i = [state[k] for k in range(3)]
    speed_i = [state[3 + k] for k in range(3)]
    turn_i = [state[6 + k] for k in range(3)]
    rad_i = radius[...]
    shear_sum = [jnp.zeros_like(rad_i) for k in range(3)]
    twist = [jnp.zeros_like(rad_i) for k in range(3)]
    for h in range(partners.shape[0]):
        code = partners[h]
        valid = code >= 0
        code = jnp.maximum(code, 0)
        which = code // slots
        member = code % slots
        picked = []
        for f in range(FIELDS):
            value = jnp.take_along_axis(around[0, f], member, axis=1)
            for n in range(1, 7):
                got = jnp.take_along_axis(around[n, f], member, axis=1)
                value = jnp.where(which == n, got, value)
            picked.append(value)
        alive = valid & (picked[9] > 0.0)
        sep = []
        for k in range(3):
            shift = jnp.where(which == 2 + 2 * k, 1.0, jnp.where(which == 1 + 2 * k, -1.0, 0.0))
            sep.append(place_i[k] - picked[k] - shift)
        distance = jnp.sqrt(sep[0] * sep[0] + sep[1] * sep[1] + sep[2] * sep[2] + soft_length**2)
        unit = [s / distance for s in sep]
        over = jnp.maximum(rad_i + picked[9] - distance, 0.0)
        root = jnp.sqrt(over)
        rel = [speed_i[k] - picked[3 + k] for k in range(3)]
        approach = rel[0] * unit[0] + rel[1] * unit[1] + rel[2] * unit[2]
        pressing = normal_stiff * over * root - normal_damp * root * approach
        lever = [rad_i * turn_i[k] + picked[9] * picked[6 + k] for k in range(3)]
        contact = [
            rel[k]
            - (
                lever[(k + 1) % 3] * unit[(k + 2) % 3]
                - lever[(k + 2) % 3] * unit[(k + 1) % 3]
            )
            for k in range(3)
        ]
        along = contact[0] * unit[0] + contact[1] * unit[1] + contact[2] * unit[2]
        old = [springs[k, h] for k in range(3)]
        old_along = old[0] * unit[0] + old[1] * unit[1] + old[2] * unit[2]
        stretched = [
            old[k] - old_along * unit[k] + time_step * (contact[k] - along * unit[k])
            for k in range(3)
        ]
        length = jnp.sqrt(
            stretched[0] * stretched[0] + stretched[1] * stretched[1] + stretched[2] * stretched[2]
        )
        limit = jnp.minimum(
            1.0, friction * jnp.abs(pressing) / jnp.maximum(shear_stiff * length, force_floor)
        )
        limit = jnp.where(alive, limit, 0.0)
        fresh = [limit * stretched[k] for k in range(3)]
        for k in range(3):
            new_springs[k, h] = fresh[k]
            shear_sum[k] = shear_sum[k] - shear_stiff * fresh[k]
            twist[k] = twist[k] - shear_stiff * (
                fresh[(k + 1) % 3] * unit[(k + 2) % 3] - fresh[(k + 2) % 3] * unit[(k + 1) % 3]
            )
    safe = jnp.where(rad_i > 0.0, rad_i, 1.0)
    ratio = safe / 0.1
    mass = ratio * ratio * ratio
    inertia = 0.4 * mass * safe * safe
    for k in range(3):
        force = normal[k] + shear_sum[k] + drag_coeff * (gas[k] - speed_i[k])
        lift = gravity if k == 2 else 0.0
        speed = speed_i[k] + time_step * (force / mass - lift)
        out[k] = place_i[k] + time_step * speed
        out[3 + k] = speed
        out[6 + k] = turn_i[k] + time_step * (rad_i * twist[k]) / inertia
    out[9] = state[9]


def middle_kernel(plan, sizes, *refs):
    n = send_count(sizes)
    state, radius, spread, inner, springs, partners, gas = refs[:7]
    halos = refs[7 : 7 + n]
    out, new_springs = refs[7 + n : 9 + n]
    sends = refs[9 + n : 9 + 2 * n]
    scratch = refs[9 + 2 * n :]
    step_core(plan, sizes, state, radius, spread, inner, springs, partners, gas, halos, out,
              new_springs, *scratch)
    put_faces(plan, sizes, out, sends)


def last_kernel(plan, sizes, *refs):
    n = send_count(sizes)
    state, radius, spread, inner, springs, partners, gas, departures = refs[:8]
    halos = refs[8 : 8 + n]
    places, speeds, turns, new_springs, out = refs[8 + n : 13 + n]
    sends = refs[13 + n : 13 + 2 * n]
    scratch = refs[13 + 2 * n :]
    step_core(plan, sizes, state, radius, spread, inner, springs, partners, gas, halos, out,
              new_springs, *scratch)
    places[...] = out[0:3]
    speeds[...] = out[3:6]
    turns[...] = out[6:9]
    slots = radius.shape[-1]
    hist = partners.shape[0]
    count = plan.count
    sub = lax.broadcasted_iota(jnp.int32, (count, slots), 0)
    values = [out[f] for f in range(9)] + [radius[...]]
    values += [new_springs[k, h] for k in range(3) for h in range(hist)]
    values += [(partners[h] + 1).astype(f32) for h in range(hist)]
    width = len(values)
    picks = [[], [], [], [], [], []]
    for d in range(6):
        leaving = jnp.broadcast_to(departures[d : d + 1, :], (count, slots))
        hit = (leaving // slots == sub) & (leaving >= 0)
        member = jnp.maximum(leaving, 0) % slots
        for v in values:
            got = jnp.where(hit, jnp.take_along_axis(v, member, axis=1), 0.0)
            picks[d].append(jnp.sum(got, axis=0, keepdims=True))
    split = per_axis(sends, sizes)
    for axis in range(3):
        for f in range(width):
            blocks = ordered_send(
                AXES[axis], sizes[axis], picks[2 * axis][f], picks[2 * axis + 1][f]
            )
            for ref, block in zip(split[axis], blocks):
                ref[f : f + 1, :] = block


def deposit_kernel(plan, sizes, *refs):
    n = send_count(sizes)
    state, radius, cells, gas, pressure, source = refs[:6]
    halos = refs[6 : 6 + n]
    force_out, pressure_out, force, new_pressure, sems = refs[6 + n :]
    copies = []

    def send(source, target):
        copies.append(pltpu.make_async_copy(source, target, sems.at[len(copies)]))
        copies[-1].start()

    slots = radius.shape[-1]
    nx, ny, nz = pressure.shape
    lanes = slots
    chunks = nz // lanes
    span = [s // d for s, d in zip(pressure.shape, plan.dims)]
    rows = span[0] * span[1]
    high_row = lax.broadcasted_iota(jnp.int32, (rows, slots), 0)
    column_row = lax.broadcasted_iota(jnp.int32, (span[2], slots), 0)
    for place in plan.places():
        b = plan.index(place)
        cell = cells[b : b + 1, :]
        live = state[9, b : b + 1, :] > 0.0
        rad = radius[b : b + 1, :]
        values = [
            jnp.where(live, drag_coeff * (state[3 + c, b : b + 1, :] - gas[c, b : b + 1, :]), 0.0)
            for c in range(3)
        ]
        values.append(jnp.where(live, 4.0 / 3.0 * math.pi * rad * rad * rad, 0.0))
        at_row = high_row == cell // span[2]
        at_column = (column_row == cell % span[2]).astype(jnp.bfloat16)
        halves = []
        for v in values:
            top = v.astype(jnp.bfloat16).astype(f32)
            left = v - top
            halves.append(
                jnp.concatenate(
                    [jnp.where(at_row, part, 0.0).astype(jnp.bfloat16) for part in (top, left)],
                    axis=1,
                )
            )
        left = jnp.concatenate(halves, axis=0)
        right = jnp.concatenate([at_column] * 2, axis=1)
        got = lax.dot_general(
            left, right, (((1,), (1,)), ((), ())), preferred_element_type=f32
        )
        x0, y0, z0 = (p * s for p, s in zip(place, span))
        block = (slice(x0, x0 + span[0]), slice(y0, y0 + span[1]), slice(z0, z0 + span[2]))
        pieces = [got[c * rows : (c + 1) * rows].reshape(span) for c in range(4)]
        for c in range(3):
            force[(c,) + block] = pieces[c]
            send(force.at[(c,) + block], force_out.at[(c,) + block])
        new_pressure[block] = volume_coeff * pieces[3] + pieces[2]
    split = per_axis(halos, sizes)
    dead = [
        [at_end(AXES[axis], sizes[axis], side) for side in (-1, 1)] for axis in range(3)
    ]
    base = FIELDS * len(plan.face(0, 1))
    slabs = []
    for ref in split[0]:
        slabs.append(
            jnp.concatenate(
                [ref[base + c * ny : base + (c + 1) * ny, :] for c in range(chunks)], axis=1
            )
        )
    x_ends = ordered_receive("gx", sizes[0], slabs)
    x_ends = [jnp.where(dead[0][s], 0.0, x_ends[s]) for s in (0, 1)]
    base = FIELDS * len(plan.face(1, 1))
    slabs = []
    for ref in split[1]:
        slabs.append(
            jnp.concatenate(
                [ref[base + c * nx : base + (c + 1) * nx, :] for c in range(chunks)], axis=1
            )
        )
    y_ends = ordered_receive("gy", sizes[1], slabs)
    y_ends = [jnp.where(dead[1][s], 0.0, y_ends[s]) for s in (0, 1)]
    base = FIELDS * len(plan.face(2, 1))
    z_ends = ordered_receive("gz", sizes[2], [ref[base : base + ny, :] for ref in split[2]])
    z_ends = [jnp.where(dead[2][s], 0.0, z_ends[s]) for s in (0, 1)]
    row = lax.broadcasted_iota(jnp.int32, (ny, nz), 0)
    column = lax.broadcasted_iota(jnp.int32, (ny, nz), 1)
    for x in range(nx):
        here = pressure[x]
        total = pressure[x - 1] if x > 0 else x_ends[0]
        total = total + (pressure[x + 1] if x < nx - 1 else x_ends[1])
        total = total + jnp.where(row == 0, y_ends[0][x : x + 1, :], pltpu.roll(here, 1, 0))
        total = total + jnp.where(
            row == ny - 1, y_ends[1][x : x + 1, :], pltpu.roll(here, ny - 1, 0)
        )
        total = total + jnp.where(column == 0, z_ends[0][:, x : x + 1], pltpu.roll(here, 1, 1))
        total = total + jnp.where(
            column == nz - 1, z_ends[1][:, x : x + 1], pltpu.roll(here, nz - 1, 1)
        )
        new_pressure[x] = (total + (source[x] + new_pressure[x])) * (1.0 / 6.0)
        if (x + 1) % span[0] == 0:
            part = slice(x + 1 - span[0], x + 1)
            send(new_pressure.at[part], pressure_out.at[part])
    for copy in copies:
        copy.wait()


def arrive_kernel(sizes, *refs):
    n = send_count(sizes)
    halos = refs[:n]
    state, codes = refs[n:]
    split = per_axis(halos, sizes)
    width = state.shape[0]
    hist = codes.shape[1]
    for axis in range(3):
        got = [ref[0 : width + hist, :] for ref in split[axis]]
        before, after = ordered_receive(AXES[axis], sizes[axis], got)
        after = jnp.where(at_end(AXES[axis], sizes[axis], 1), 0.0, after)
        before = jnp.where(at_end(AXES[axis], sizes[axis], -1), 0.0, before)
        for d, block in ((2 * axis, after), (2 * axis + 1, before)):
            state[:, d, 0, :] = block[0:width]
            codes[d] = block[width : width + hist].astype(jnp.int32) - 1


def call(kernel, outs, scratch, args, hbm=(), flops=0, outs_hbm=False):
    specs = []
    args = [
        pltpu.with_memory_space_constraint(a, pltpu.HBM) if k in hbm else a
        for k, a in enumerate(args)
    ]
    for k in range(len(args)):
        space = pltpu.HBM if k in hbm else pltpu.VMEM
        specs.append(pl.BlockSpec(memory_space=space))
    return pl.pallas_call(
        kernel,
        out_shape=[jax.ShapeDtypeStruct(s, d) for s, d in outs],
        in_specs=specs,
        out_specs=[pl.BlockSpec(memory_space=pltpu.HBM if outs_hbm else pltpu.VMEM)] * len(outs),
        scratch_shapes=scratch,
        compiler_params=pltpu.CompilerParams(vmem_limit_bytes=32 * 1024 * 1024),
        cost_estimate=pl.CostEstimate(flops=flops, bytes_accessed=1 << 20, transcendentals=0),
    )(*args)


def body(sizes, positions, velocities, spins, radii, counts, springs, partners, cells, departures,
         fluid_velocity, pressure, pressure_source):
    plan = Plan(radii.shape[:3])
    count = plan.count
    slots = radii.shape[3]
    hist = partners.shape[0]
    nx, ny, nz = pressure.shape
    chunks = nz // slots
    flat = lambda a: a.reshape(a.shape[:-4] + (count, slots))
    pos, vel, spin = flat(positions), flat(velocities), flat(spins)
    radius = radii.reshape(count, slots)
    springs = springs.reshape(3, hist, count, slots)
    partners = partners.reshape(hist, count, slots)
    cells = cells.reshape(count, slots)
    leaving = departures.reshape(6, slots)

    faces = [FIELDS * len(plan.face(a, 1)) for a in range(3)]
    extra = [chunks * ny, chunks * nx, ny]
    vm = lambda *s: pltpu.VMEM(s, f32)

    def sends(rows):
        out = []
        for a in range(3):
            for _ in rolls(AXES[a], sizes):
                out.append(((rows[a], slots), f32))
        return out

    inside = [sum(plan.neighbour(p, n)[0] for n in range(7)) for p in plan.places()]

    def pair_scratch(jobs):
        return [vm(jobs + 2, 8, slots), pltpu.SMEM((jobs + 8,), jnp.int32)]

    own_scratch = [vm(count, 8, slots)] + pair_scratch(sum(inside))
    spread_shape = ((count, 7, slots, slots), f32)
    parts_shape = ((count, 3, slots, slots), f32)
    step_scratch = [vm(7, FIELDS, count, slots)] + pair_scratch(7 * count - sum(inside))
    step_scratch.append(vm(count, 3, slots, slots))
    state_shape = ((FIELDS, count, slots), f32)
    three = ((3, count, slots), f32)
    spring_shape = ((3, hist, count, slots), f32)
    bind = functools.partial

    state, radius, *out = call(
        bind(pack_kernel, plan, sizes),
        [state_shape, ((count, slots), f32)] + sends([f + e for f, e in zip(faces, extra)]),
        [
            pltpu.VMEM(counts.shape, jnp.int32),
            vm(nx, ny, nz),
            pltpu.SemaphoreType.DMA((6,)),
        ],
        [pos, vel, spin, radius, counts, pressure],
        hbm=(0, 1, 2, 3, 4, 5),
        flops=1 << 20,
    )
    first_halos = exchange(out, sizes)
    spread, inner, gas, cells = call(
        bind(inner_kernel, plan, True),
        [spread_shape, parts_shape, three, ((count, slots), jnp.int32)],
        own_scratch + [vm(3, nx, ny, nz), pltpu.SemaphoreType.DMA((2,))],
        [state, radius, cells, fluid_velocity],
        hbm=(2, 3),
        flops=1 << 25,
    )
    state, springs, *out = call(
        bind(middle_kernel, plan, sizes),
        [state_shape, spring_shape] + sends(faces),
        step_scratch,
        [state, radius, spread, inner, springs, partners, gas] + first_halos,
        flops=1 << 25,
    )
    halos = exchange(out, sizes)
    spread, inner = call(
        bind(inner_kernel, plan, False), [spread_shape, parts_shape], own_scratch,
        [state, radius], flops=1 << 25
    )
    width = 10 + 4 * hist
    padded = (width + 7) // 8 * 8
    places, speeds, turns, springs, state, *out = call(
        bind(last_kernel, plan, sizes),
        [three, three, three, spring_shape, state_shape] + sends([padded] * 3),
        step_scratch,
        [state, radius, spread, inner, springs, partners, gas, leaving] + halos,
        flops=1 << 25,
    )
    arrivals = exchange(out, sizes)
    force, new_pressure = call(
        bind(deposit_kernel, plan, sizes),
        [((3, nx, ny, nz), f32), ((nx, ny, nz), f32)],
        [
            vm(3, nx, ny, nz),
            vm(nx, ny, nz),
            pltpu.SemaphoreType.DMA((3 * count + plan.dims[0],)),
        ],
        [state, radius, cells, gas, pressure, pressure_source] + first_halos,
        outs_hbm=True,
        flops=1 << 25,
    )
    arrived, arrived_partners = call(
        bind(arrive_kernel, sizes),
        [((10 + 3 * hist, 6, 1, slots), f32), ((6, hist, slots), jnp.int32)],
        [],
        arrivals,
        flops=1 << 20,
    )
    wide = lambda a: a.reshape(a.shape[:-2] + radii.shape)
    return (
        wide(places),
        wide(speeds),
        wide(turns),
        wide(springs),
        force,
        new_pressure,
        arrived.reshape(1, 1, 1, 10 + 3 * hist, 6, slots),
        jnp.transpose(arrived_partners, (1, 0, 2))[None, None, None],
    )


def solution(mesh):
    sizes = tuple(mesh.shape[a] for a in AXES)
    return jax.shard_map(
        functools.partial(body, sizes),
        mesh=mesh,
        in_specs=(
            P(None, "gx", "gy", "gz", None),
            P(None, "gx", "gy", "gz", None),
            P(None, "gx", "gy", "gz", None),
            P("gx", "gy", "gz", None),
            P("gx", "gy", "gz"),
            P(None, None, "gx", "gy", "gz", None),
            P(None, "gx", "gy", "gz", None),
            P("gx", "gy", "gz", None),
            P("gx", "gy", "gz", None, None),
            P(None, "gx", "gy", "gz"),
            P("gx", "gy", "gz"),
            P("gx", "gy", "gz"),
        ),
        out_specs=(
            P(None, "gx", "gy", "gz", None),
            P(None, "gx", "gy", "gz", None),
            P(None, "gx", "gy", "gz", None),
            P(None, None, "gx", "gy", "gz", None),
            P(None, "gx", "gy", "gz"),
            P("gx", "gy", "gz"),
            P("gx", "gy", "gz", None, None, None),
            P("gx", "gy", "gz", None, None, None),
        ),
        check_vma=False,
    )
```

```python
import functools
import math

import jax
import jax.numpy as jnp
from jax import lax
from jax.experimental import pallas as pl
from jax.experimental.pallas import tpu as pltpu
from jax.sharding import PartitionSpec as P

SUBSTEPS = 2

normal_stiff = 100.0
normal_damp = 2.0
shear_stiff = 30.0
friction = 0.5
time_step = 0.05
drag_coeff = 0.8
gravity = 1.0
soft_length = 0.05
force_floor = 0.5
volume_coeff = 100.0
neighbours = ((0, 0, 0), (-1, 0, 0), (1, 0, 0), (0, -1, 0), (0, 1, 0), (0, 0, -1), (0, 0, 1))
AXES = ("gx", "gy", "gz")
FIELDS = 10
DEAD = -8.0
TINY = 1e-30
f32 = jnp.float32


class Plan:
    def __init__(self, shape):
        self.dims = shape
        self.count = shape[0] * shape[1] * shape[2]

    def index(self, place):
        return (place[0] * self.dims[1] + place[1]) * self.dims[2] + place[2]

    def places(self):
        d = self.dims
        return [(a, b, c) for a in range(d[0]) for b in range(d[1]) for c in range(d[2])]

    def face(self, axis, side):
        edge = self.dims[axis] - 1 if side > 0 else 0
        return [self.index(p) for p in self.places() if p[axis] == edge]

    def neighbour(self, place, number):
        move = neighbours[number]
        other = tuple(p + m for p, m in zip(place, move))
        if all(0 <= o < d for o, d in zip(other, self.dims)):
            return True, self.index(other)
        axis = (number - 1) // 2
        across = [o for k, o in enumerate(place) if k != axis]
        width = [d for k, d in enumerate(self.dims) if k != axis][1]
        return False, across[0] * width + across[1]


def rolls(axis, sizes):
    size = sizes[AXES.index(axis)]
    if is_ring(axis, size):
        return [
            (axis, [(i, (i + 1) % size) for i in range(size)]),
            (axis, [((i + 1) % size, i) for i in range(size)]),
        ]

    def swaps(start):
        pairs = []
        for i in range(start, size - 1, 2):
            pairs += [(i, i + 1), (i + 1, i)]
        return pairs

    out = [(axis, swaps(0))]
    if size > 2:
        pairs = swaps(1)
        inside = [i for i, _ in pairs]
        across = sizes[0]
        if axis != "gx" and across % 2 == 0:
            joint = []
            for x in range(across):
                joint += [(x * size + i, x * size + j) for i, j in pairs]
                joint += [(x * size + i, (x ^ 1) * size + i) for i in range(size) if i not in inside]
            out.append((("gx", axis), joint))
        else:
            out.append((axis, pairs))
    return out


def is_ring(axis, size):
    return axis == "gx" and size > 2


def ordered_send(axis, size, low, high):
    if is_ring(axis, size):
        return [high, low]
    even = lax.axis_index(axis) % 2 == 0
    first = jnp.where(even, high, low)
    if size == 2:
        return [first]
    return [first, jnp.where(even, low, high)]


def ordered_receive(axis, size, blocks):
    if is_ring(axis, size):
        return blocks[0], blocks[1]
    if size == 2:
        return blocks[0], blocks[0]
    even = lax.axis_index(axis) % 2 == 0
    return jnp.where(even, blocks[1], blocks[0]), jnp.where(even, blocks[0], blocks[1])


def at_end(axis, size, side):
    edge = size - 1 if side > 0 else 0
    return lax.axis_index(axis) == edge


START_ORDER = (3, 2, 4, 1, 0)


def start_order(sizes):
    count = send_count(sizes)
    return START_ORDER if count == len(START_ORDER) else tuple(range(count))


def exchange(blocks, sizes):
    routes = [route for axis in AXES for route in rolls(axis, sizes)]
    routes = [routes[k] for k in start_order(sizes)]
    return [lax.ppermute(block, axes, pairs) for block, (axes, pairs) in zip(blocks, routes)]


def per_axis(refs, sizes):
    sorted_refs = [None] * len(refs)
    for ref, k in zip(refs, start_order(sizes)):
        sorted_refs[k] = ref
    out = []
    k = 0
    for axis in AXES:
        n = len(rolls(axis, sizes))
        out.append(sorted_refs[k : k + n])
        k += n
    return out


def send_count(sizes):
    return sum(len(rolls(a, sizes)) for a in AXES)


def put_faces(plan, sizes, state_ref, send_refs):
    for axis, refs in enumerate(per_axis(send_refs, sizes)):
        low = plan.face(axis, -1)
        high = plan.face(axis, 1)
        width = len(low)
        for k in range(width):
            a = state_ref[:, low[k], :]
            b = state_ref[:, high[k], :]
            for ref, block in zip(refs, ordered_send(AXES[axis], sizes[axis], a, b)):
                ref[pl.ds(k, FIELDS, stride=width), :] = block


def pack_kernel(plan, sizes, pos, vel, spin, rad, counts_hbm, *refs):
    state, radius = refs[:2]
    sends = refs[2:-2]
    counts, sems = refs[-2:]
    copies = [
        pltpu.make_async_copy(rad, radius, sems.at[0]),
        pltpu.make_async_copy(pos, state.at[0:3], sems.at[1]),
        pltpu.make_async_copy(vel, state.at[3:6], sems.at[2]),
        pltpu.make_async_copy(spin, state.at[6:9], sems.at[3]),
        pltpu.make_async_copy(counts_hbm, counts, sems.at[4]),
    ]
    for copy in copies:
        copy.start()
    slots = rad.shape[-1]
    lane = lax.broadcasted_iota(jnp.int32, (1, slots), 1)
    places = plan.places()
    for copy in copies:
        copy.wait()
    for b in range(plan.count):
        x, y, z = places[b]
        live = lane < counts[x, y : y + 1, z : z + 1]
        state[9, b : b + 1, :] = jnp.where(live, radius[b : b + 1, :], DEAD)
    put_faces(plan, sizes, state, sends)


def put_pressure(plan, sizes, lanes, pressure, sends):
    nx, ny, nz = pressure.shape
    chunks = nz // lanes
    split = per_axis(sends, sizes)
    base = FIELDS * len(plan.face(0, 1))
    for ref, block in zip(
        split[0], ordered_send("gx", sizes[0], pressure[0], pressure[nx - 1])
    ):
        for c in range(chunks):
            ref[base + c * ny : base + (c + 1) * ny, :] = block[:, c * lanes : (c + 1) * lanes]
    base = FIELDS * len(plan.face(1, 1))
    for ref, block in zip(
        split[1], ordered_send("gy", sizes[1], pressure[:, 0, :], pressure[:, ny - 1, :])
    ):
        for c in range(chunks):
            ref[base + c * nx : base + (c + 1) * nx, :] = block[:, c * lanes : (c + 1) * lanes]
    base = FIELDS * len(plan.face(2, 1))
    wide = lax.broadcasted_iota(jnp.int32, (ny, lanes), 1)
    low = jnp.zeros((ny, lanes), f32)
    high = jnp.zeros((ny, lanes), f32)
    for x in range(nx):
        low = jnp.where(wide == x, jnp.broadcast_to(pressure[x, :, 0:1], (ny, lanes)), low)
        high = jnp.where(
            wide == x, jnp.broadcast_to(pressure[x, :, nz - 1 : nz], (ny, lanes)), high
        )
    for ref, block in zip(split[2], ordered_send("gz", sizes[2], low, high)):
        ref[base : base + ny, :] = block


def pair_rows(state, radius, mine):
    scale = normal_damp / normal_stiff
    for k in range(3):
        mine[:, k, :] = state[k]
        mine[:, 3 + k, :] = state[3 + k] * scale
    mine[:, 6, :] = radius[...]
    mine[:, 7, :] = radius[...]


def spread_rows(mine, spread):
    bins, fields, slots = mine.shape
    part = lax.broadcasted_iota(jnp.int32, (3 * fields, 7 * slots), 0) % fields
    block = lax.broadcasted_iota(jnp.int32, (3 * fields, 7 * slots), 1) // slots
    ones = (part == block).astype(jnp.bfloat16)
    for b in range(bins):
        rows = mine[b]
        top = rows.astype(jnp.bfloat16).astype(f32)
        left = rows - top
        mid = left.astype(jnp.bfloat16).astype(f32)
        parts = jnp.concatenate([top, mid, left - mid], axis=0).astype(jnp.bfloat16)
        wide = lax.dot_general(
            parts, ones, (((0,), (0,)), ((), ())), preferred_element_type=f32
        )
        for f in range(7):
            spread[b, f] = wide[:, f * slots : (f + 1) * slots]


def list_pairs(plan, entries, packed, table):
    slots = packed.shape[-1]
    lane = lax.broadcasted_iota(jnp.int32, (8, slots), 1)
    field = lax.broadcasted_iota(jnp.int32, (8, slots), 0)
    empty = jnp.where(field == 6, DEAD, 0.0)
    jobs = jnp.int32(0)
    for b in range(plan.count):
        start = jobs
        at = None
        for rows, count, move in entries[b]:
            value = rows
            for k in range(3):
                if move[k]:
                    value = value + jnp.where(field == k, float(move[k]), 0.0)
            if at is None:
                packed[start] = jnp.where(lane < count, value, empty)
                packed[start + 1] = empty
                at = count
                continue
            shift = at % slots
            job = start + at // slots
            moved = pltpu.roll(value, shift, 1)
            packed[job] = jnp.where(
                (lane >= shift) & (lane < shift + count), moved, packed[job]
            )
            packed[job + 1] = jnp.where(lane < shift + count - slots, moved, empty)
            at = at + count
        jobs = start + (at + slots - 1) // slots
        for q in range(len(entries[b])):
            table[start + q] = b
    return jobs


def run_pairs(jobs, spread, packed, table, parts):
    slots = packed.shape[-1]

    def job(t, carry):
        b = table[t]
        their = [jnp.broadcast_to(packed[t, f : f + 1, :], (8, slots)) for f in range(7)]
        for tile in range(slots // 8):
            rows = slice(tile * 8, tile * 8 + 8)
            own = [spread[b, f, rows, :] for f in range(7)]
            sep = [own[k] - their[k] for k in range(3)]
            square = sep[0] * sep[0] + (sep[1] * sep[1] + (sep[2] * sep[2] + soft_length**2))
            inverse = lax.rsqrt(square)
            over = (own[6] + their[6]) - square * inverse
            positive = jnp.maximum(over, 0.0)
            root = positive * lax.rsqrt(jnp.maximum(over, TINY))
            dot = (own[3] - their[3]) * sep[0]
            dot = dot + (own[4] - their[4]) * sep[1]
            dot = dot + (own[5] - their[5]) * sep[2]
            weight = (positive - dot * inverse) * (root * inverse)
            for k in range(3):
                parts[b, k, rows, :] = parts[b, k, rows, :] + weight * sep[k]
        return carry

    lax.fori_loop(0, jobs, job, 0)


def inner_kernel(plan, with_fluid, *refs):
    if with_fluid:
        (state, radius, cells_hbm, fluid_hbm, spread, parts, gas, cells, mine, packed,
         table, fluid, sems) = refs
        fetches = [
            pltpu.make_async_copy(cells_hbm, cells, sems.at[0]),
            pltpu.make_async_copy(fluid_hbm, fluid, sems.at[1]),
        ]
        for fetch in fetches:
            fetch.start()
    else:
        state, radius, spread, parts, mine, packed, table = refs
    parts[...] = jnp.zeros_like(parts)
    pair_rows(state, radius, mine)
    spread_rows(mine, spread)
    records = []
    for b in range(plan.count):
        rows = mine[b]
        field = lax.broadcasted_iota(jnp.int32, rows.shape, 0)
        records.append(jnp.where(field == 6, state[9, b : b + 1, :], rows))
    filled = jnp.sum(jnp.where(state[9] > 0.0, 1, 0), axis=1, keepdims=True)
    entries = []
    for place in plan.places():
        entry = []
        for n in range(7):
            own, other = plan.neighbour(place, n)
            if own:
                entry.append((records[other], filled[other, 0], neighbours[n]))
        entries.append(entry)
    jobs = list_pairs(plan, entries, packed, table)
    run_pairs(jobs, spread, packed, table, parts)
    if not with_fluid:
        return
    for fetch in fetches:
        fetch.wait()
    slots = radius.shape[-1]
    span = [s // d for s, d in zip(fluid.shape[1:], plan.dims)]
    sub = lax.broadcasted_iota(jnp.int32, (8, slots), 0)
    for place in plan.places():
        b = plan.index(place)
        cell = cells[b : b + 1, :]
        column = jnp.broadcast_to(cell % span[2], (8, slots))
        row = jnp.broadcast_to(cell // span[2], (8, slots)) - sub
        sums_c = [jnp.zeros((8, slots), f32) for c in range(3)]
        for a in range(span[0]):
            for h in range(span[1] // 8):
                hit = row == a * span[1] + h * 8
                y0 = place[1] * span[1] + h * 8
                z0 = place[2] * span[2]
                for c in range(3):
                    block = fluid[c, place[0] * span[0] + a, y0 : y0 + 8, z0 : z0 + span[2]]
                    got = jnp.take_along_axis(block, column, axis=1)
                    sums_c[c] = jnp.where(hit, got, sums_c[c])
        for c in range(3):
            gas[c, b : b + 1, :] = jnp.sum(sums_c[c], axis=0, keepdims=True)


def step_core(plan, sizes, state, radius, spread, inner, springs, partners, gas, halos, out,
              new_springs, around, packed, table, parts):
    scale = normal_damp / normal_stiff
    places = plan.places()
    slots = radius.shape[-1]
    split = per_axis(halos, sizes)
    around[0] = state[...]
    for axis in range(3):
        width = len(plan.face(axis, 1))
        for place in places:
            b = plan.index(place)
            for side in (0, 1):
                n = 1 + 2 * axis + side
                own, other = plan.neighbour(place, n)
                if own:
                    around[n, :, b, :] = state[:, other, :]
                    continue
                got = [ref[pl.ds(other, FIELDS, stride=width), :] for ref in split[axis]]
                before, after = ordered_receive(AXES[axis], sizes[axis], got)
                around[n, :, b, :] = after if side else before
    sub = lax.broadcasted_iota(jnp.int32, (plan.count, slots), 0)
    inner_count = [plan.dims[1] * plan.dims[2], plan.dims[2], 1]
    entries = [[] for _ in places]
    parts[...] = inner[...]
    for n in range(1, 7):
        axis = (n - 1) // 2
        side = 1 if n % 2 == 0 else -1
        edge = plan.dims[axis] - 1 if side > 0 else 0
        level = sub // inner_count[axis] % plan.dims[axis]
        gone = at_end(AXES[axis], sizes[axis], side)
        reach = around[n, 9]
        reach = jnp.where(((level == edge) & gone) | (reach <= 0.0), DEAD, reach)
        around[n, 9] = reach
        filled = jnp.sum(jnp.where(reach > 0.0, 1, 0), axis=1, keepdims=True)
        for place in places:
            b = plan.index(place)
            if plan.neighbour(place, n)[0]:
                continue
            rows = around[n, 0:8, b, :]
            field = lax.broadcasted_iota(jnp.int32, rows.shape, 0)
            rows = jnp.where((field > 2) & (field < 6), rows * scale, rows)
            rows = jnp.where(field == 6, reach[b : b + 1, :], rows)
            entries[b].append((rows, filled[b, 0], neighbours[n]))
    jobs = list_pairs(plan, entries, packed, table)
    run_pairs(jobs, spread, packed, table, parts)
    normal = []
    for k in range(3):
        sums = [
            jnp.sum(jnp.transpose(parts[b, k], (1, 0)), axis=0, keepdims=True)
            for b in range(plan.count)
        ]
        normal.append(jnp.concatenate(sums, axis=0) * normal_stiff)
    place_i = [state[k] for k in range(3)]
    speed_i = [state[3 + k] for k in range(3)]
    turn_i = [state[6 + k] for k in range(3)]
    rad_i = radius[...]
    shear_sum = [jnp.zeros_like(rad_i) for k in range(3)]
    twist = [jnp.zeros_like(rad_i) for k in range(3)]
    for h in range(partners.shape[0]):
        code = partners[h]
        valid = code >= 0
        code = jnp.maximum(code, 0)
        which = code // slots
        member = code % slots
        picked = []
        for f in range(FIELDS):
            value = jnp.take_along_axis(around[0, f], member, axis=1)
            for n in range(1, 7):
                got = jnp.take_along_axis(around[n, f], member, axis=1)
                value = jnp.where(which == n, got, value)
            picked.append(value)
        alive = valid & (picked[9] > 0.0)
        sep = []
        for k in range(3):
            shift = jnp.where(which == 2 + 2 * k, 1.0, jnp.where(which == 1 + 2 * k, -1.0, 0.0))
            sep.append(place_i[k] - picked[k] - shift)
        distance = jnp.sqrt(sep[0] * sep[0] + sep[1] * sep[1] + sep[2] * sep[2] + soft_length**2)
        unit = [s / distance for s in sep]
        over = jnp.maximum(rad_i + picked[9] - distance, 0.0)
        root = jnp.sqrt(over)
        rel = [speed_i[k] - picked[3 + k] for k in range(3)]
        approach = rel[0] * unit[0] + rel[1] * unit[1] + rel[2] * unit[2]
        pressing = normal_stiff * over * root - normal_damp * root * approach
        lever = [rad_i * turn_i[k] + picked[9] * picked[6 + k] for k in range(3)]
        contact = [
            rel[k]
            - (
                lever[(k + 1) % 3] * unit[(k + 2) % 3]
                - lever[(k + 2) % 3] * unit[(k + 1) % 3]
            )
            for k in range(3)
        ]
        along = contact[0] * unit[0] + contact[1] * unit[1] + contact[2] * unit[2]
        old = [springs[k, h] for k in range(3)]
        old_along = old[0] * unit[0] + old[1] * unit[1] + old[2] * unit[2]
        stretched = [
            old[k] - old_along * unit[k] + time_step * (contact[k] - along * unit[k])
            for k in range(3)
        ]
        length = jnp.sqrt(
            stretched[0] * stretched[0] + stretched[1] * stretched[1] + stretched[2] * stretched[2]
        )
        limit = jnp.minimum(
            1.0, friction * jnp.abs(pressing) / jnp.maximum(shear_stiff * length, force_floor)
        )
        limit = jnp.where(alive, limit, 0.0)
        fresh = [limit * stretched[k] for k in range(3)]
        for k in range(3):
            new_springs[k, h] = fresh[k]
            shear_sum[k] = shear_sum[k] - shear_stiff * fresh[k]
            twist[k] = twist[k] - shear_stiff * (
                fresh[(k + 1) % 3] * unit[(k + 2) % 3] - fresh[(k + 2) % 3] * unit[(k + 1) % 3]
            )
    safe = jnp.where(rad_i > 0.0, rad_i, 1.0)
    ratio = safe / 0.1
    mass = ratio * ratio * ratio
    inertia = 0.4 * mass * safe * safe
    for k in range(3):
        force = normal[k] + shear_sum[k] + drag_coeff * (gas[k] - speed_i[k])
        lift = gravity if k == 2 else 0.0
        speed = speed_i[k] + time_step * (force / mass - lift)
        out[k] = place_i[k] + time_step * speed
        out[3 + k] = speed
        out[6 + k] = turn_i[k] + time_step * (rad_i * twist[k]) / inertia
    out[9] = state[9]


def middle_kernel(plan, sizes, *refs):
    n = send_count(sizes)
    state, radius, spread, inner, springs, partners, gas, pressure = refs[:8]
    halos = refs[8 : 8 + n]
    out, new_springs = refs[8 + n : 10 + n]
    sends = refs[10 + n : 10 + 2 * n]
    scratch = refs[10 + 2 * n :]
    put_pressure(plan, sizes, radius.shape[-1], pressure, sends)
    step_core(plan, sizes, state, radius, spread, inner, springs, partners, gas, halos, out,
              new_springs, *scratch)
    put_faces(plan, sizes, out, sends)


def last_kernel(plan, sizes, *refs):
    n = send_count(sizes)
    state, radius, spread, inner, springs, partners, gas, departures = refs[:8]
    halos = refs[8 : 8 + n]
    places, speeds, turns, new_springs, out = refs[8 + n : 13 + n]
    sends = refs[13 + n : 13 + 2 * n]
    scratch = refs[13 + 2 * n :]
    step_core(plan, sizes, state, radius, spread, inner, springs, partners, gas, halos, out,
              new_springs, *scratch)
    places[...] = out[0:3]
    speeds[...] = out[3:6]
    turns[...] = out[6:9]
    slots = radius.shape[-1]
    hist = partners.shape[0]
    count = plan.count
    sub = lax.broadcasted_iota(jnp.int32, (count, slots), 0)
    values = [out[f] for f in range(9)] + [radius[...]]
    values += [new_springs[k, h] for k in range(3) for h in range(hist)]
    values += [(partners[h] + 1).astype(f32) for h in range(hist)]
    width = len(values)
    picks = [[], [], [], [], [], []]
    for d in range(6):
        leaving = jnp.broadcast_to(departures[d : d + 1, :], (count, slots))
        hit = (leaving // slots == sub) & (leaving >= 0)
        member = jnp.maximum(leaving, 0) % slots
        for v in values:
            got = jnp.where(hit, jnp.take_along_axis(v, member, axis=1), 0.0)
            picks[d].append(jnp.sum(got, axis=0, keepdims=True))
    split = per_axis(sends, sizes)
    for axis in range(3):
        for f in range(width):
            blocks = ordered_send(
                AXES[axis], sizes[axis], picks[2 * axis][f], picks[2 * axis + 1][f]
            )
            for ref, block in zip(split[axis], blocks):
                ref[f : f + 1, :] = block


def deposit_kernel(plan, sizes, *refs):
    n = send_count(sizes)
    state, radius, cells, gas, pressure, source = refs[:6]
    halos = refs[6 : 6 + n]
    force_out, pressure_out, force, new_pressure, sems = refs[6 + n :]
    copies = []

    def send(source, target):
        copies.append(pltpu.make_async_copy(source, target, sems.at[len(copies)]))
        copies[-1].start()

    slots = radius.shape[-1]
    nx, ny, nz = pressure.shape
    lanes = slots
    chunks = nz // lanes
    span = [s // d for s, d in zip(pressure.shape, plan.dims)]
    rows = span[0] * span[1]
    high_row = lax.broadcasted_iota(jnp.int32, (rows, slots), 0)
    column_row = lax.broadcasted_iota(jnp.int32, (span[2], slots), 0)
    def deposit(place):
        b = plan.index(place)
        cell = cells[b : b + 1, :]
        live = state[9, b : b + 1, :] > 0.0
        rad = radius[b : b + 1, :]
        values = [
            jnp.where(live, drag_coeff * (state[3 + c, b : b + 1, :] - gas[c, b : b + 1, :]), 0.0)
            for c in range(3)
        ]
        values.append(jnp.where(live, 4.0 / 3.0 * math.pi * rad * rad * rad, 0.0))
        at_row = high_row == cell // span[2]
        at_column = (column_row == cell % span[2]).astype(jnp.bfloat16)
        halves = []
        for v in values:
            top = v.astype(jnp.bfloat16).astype(f32)
            left = v - top
            halves.append(
                jnp.concatenate(
                    [jnp.where(at_row, part, 0.0).astype(jnp.bfloat16) for part in (top, left)],
                    axis=1,
                )
            )
        left = jnp.concatenate(halves, axis=0)
        right = jnp.concatenate([at_column] * 2, axis=1)
        got = lax.dot_general(
            left, right, (((1,), (1,)), ((), ())), preferred_element_type=f32
        )
        x0, y0, z0 = (p * s for p, s in zip(place, span))
        block = (slice(x0, x0 + span[0]), slice(y0, y0 + span[1]), slice(z0, z0 + span[2]))
        pieces = [got[c * rows : (c + 1) * rows].reshape(span) for c in range(4)]
        for c in range(3):
            force[(c,) + block] = pieces[c]
        new_pressure[block] = volume_coeff * pieces[3] + pieces[2]
    split = per_axis(halos, sizes)
    dead = [
        [at_end(AXES[axis], sizes[axis], side) for side in (-1, 1)] for axis in range(3)
    ]
    base = FIELDS * len(plan.face(0, 1))
    slabs = []
    for ref in split[0]:
        slabs.append(
            jnp.concatenate(
                [ref[base + c * ny : base + (c + 1) * ny, :] for c in range(chunks)], axis=1
            )
        )
    x_ends = ordered_receive("gx", sizes[0], slabs)
    x_ends = [jnp.where(dead[0][s], 0.0, x_ends[s]) for s in (0, 1)]
    base = FIELDS * len(plan.face(1, 1))
    slabs = []
    for ref in split[1]:
        slabs.append(
            jnp.concatenate(
                [ref[base + c * nx : base + (c + 1) * nx, :] for c in range(chunks)], axis=1
            )
        )
    y_ends = ordered_receive("gy", sizes[1], slabs)
    y_ends = [jnp.where(dead[1][s], 0.0, y_ends[s]) for s in (0, 1)]
    base = FIELDS * len(plan.face(2, 1))
    z_ends = ordered_receive("gz", sizes[2], [ref[base : base + ny, :] for ref in split[2]])
    z_ends = [jnp.where(dead[2][s], 0.0, z_ends[s]) for s in (0, 1)]
    row = lax.broadcasted_iota(jnp.int32, (ny, nz), 0)
    column = lax.broadcasted_iota(jnp.int32, (ny, nz), 1)
    def sweep(x):
        here = pressure[x]
        total = pressure[x - 1] if x > 0 else x_ends[0]
        total = total + (pressure[x + 1] if x < nx - 1 else x_ends[1])
        total = total + jnp.where(row == 0, y_ends[0][x : x + 1, :], pltpu.roll(here, 1, 0))
        total = total + jnp.where(
            row == ny - 1, y_ends[1][x : x + 1, :], pltpu.roll(here, ny - 1, 0)
        )
        total = total + jnp.where(column == 0, z_ends[0][:, x : x + 1], pltpu.roll(here, 1, 1))
        total = total + jnp.where(
            column == nz - 1, z_ends[1][:, x : x + 1], pltpu.roll(here, nz - 1, 1)
        )
        new_pressure[x] = (total + (source[x] + new_pressure[x])) * (1.0 / 6.0)

    layers = plan.dims[0]
    for layer in range(layers + 1):
        if layer < layers:
            for place in plan.places():
                if place[0] == layer:
                    deposit(place)
        if layer > 0:
            for x in range((layer - 1) * span[0], layer * span[0]):
                sweep(x)
        if layer < layers:
            part = slice(layer * span[0], (layer + 1) * span[0])
            for c in range(3):
                send(force.at[c, part], force_out.at[c, part])
        if layer > 0:
            part = slice((layer - 1) * span[0], layer * span[0])
            send(new_pressure.at[part], pressure_out.at[part])
    for copy in copies:
        copy.wait()


def arrive_kernel(sizes, *refs):
    n = send_count(sizes)
    halos = refs[:n]
    state, codes = refs[n:]
    split = per_axis(halos, sizes)
    width = state.shape[0]
    hist = codes.shape[1]
    for axis in range(3):
        got = [ref[0 : width + hist, :] for ref in split[axis]]
        before, after = ordered_receive(AXES[axis], sizes[axis], got)
        after = jnp.where(at_end(AXES[axis], sizes[axis], 1), 0.0, after)
        before = jnp.where(at_end(AXES[axis], sizes[axis], -1), 0.0, before)
        for d, block in ((2 * axis, after), (2 * axis + 1, before)):
            state[:, d, 0, :] = block[0:width]
            codes[d] = block[width : width + hist].astype(jnp.int32) - 1


def call(kernel, outs, scratch, args, hbm=(), flops=0, outs_hbm=False):
    specs = []
    args = [
        pltpu.with_memory_space_constraint(a, pltpu.HBM) if k in hbm else a
        for k, a in enumerate(args)
    ]
    for k in range(len(args)):
        space = pltpu.HBM if k in hbm else pltpu.VMEM
        specs.append(pl.BlockSpec(memory_space=space))
    return pl.pallas_call(
        kernel,
        out_shape=[jax.ShapeDtypeStruct(s, d) for s, d in outs],
        in_specs=specs,
        out_specs=[pl.BlockSpec(memory_space=pltpu.HBM if outs_hbm else pltpu.VMEM)] * len(outs),
        scratch_shapes=scratch,
        compiler_params=pltpu.CompilerParams(vmem_limit_bytes=32 * 1024 * 1024),
        cost_estimate=pl.CostEstimate(flops=flops, bytes_accessed=1 << 20, transcendentals=0),
    )(*args)


def body(sizes, positions, velocities, spins, radii, counts, springs, partners, cells, departures,
         fluid_velocity, pressure, pressure_source):
    plan = Plan(radii.shape[:3])
    count = plan.count
    slots = radii.shape[3]
    hist = partners.shape[0]
    nx, ny, nz = pressure.shape
    chunks = nz // slots
    flat = lambda a: a.reshape(a.shape[:-4] + (count, slots))
    pos, vel, spin = flat(positions), flat(velocities), flat(spins)
    radius = radii.reshape(count, slots)
    springs = springs.reshape(3, hist, count, slots)
    partners = partners.reshape(hist, count, slots)
    cells = cells.reshape(count, slots)
    leaving = departures.reshape(6, slots)

    faces = [FIELDS * len(plan.face(a, 1)) for a in range(3)]
    extra = [chunks * ny, chunks * nx, ny]
    vm = lambda *s: pltpu.VMEM(s, f32)

    def sends(rows):
        out = []
        for a in range(3):
            for _ in rolls(AXES[a], sizes):
                out.append(((rows[a], slots), f32))
        return [out[k] for k in start_order(sizes)]

    inside = [sum(plan.neighbour(p, n)[0] for n in range(7)) for p in plan.places()]

    def pair_scratch(jobs):
        return [vm(jobs + 2, 8, slots), pltpu.SMEM((jobs + 8,), jnp.int32)]

    own_scratch = [vm(count, 8, slots)] + pair_scratch(sum(inside))
    spread_shape = ((count, 7, slots, slots), f32)
    parts_shape = ((count, 3, slots, slots), f32)
    step_scratch = [vm(7, FIELDS, count, slots)] + pair_scratch(7 * count - sum(inside))
    step_scratch.append(vm(count, 3, slots, slots))
    state_shape = ((FIELDS, count, slots), f32)
    three = ((3, count, slots), f32)
    spring_shape = ((3, hist, count, slots), f32)
    bind = functools.partial

    state, radius, *out = call(
        bind(pack_kernel, plan, sizes),
        [state_shape, ((count, slots), f32)] + sends(faces),
        [
            pltpu.VMEM(counts.shape, jnp.int32),
            pltpu.SemaphoreType.DMA((5,)),
        ],
        [pos, vel, spin, radius, counts],
        hbm=(0, 1, 2, 3, 4),
        flops=1 << 20,
    )
    first_halos = exchange(out, sizes)
    spread, inner, gas, cells = call(
        bind(inner_kernel, plan, True),
        [spread_shape, parts_shape, three, ((count, slots), jnp.int32)],
        own_scratch + [vm(3, nx, ny, nz), pltpu.SemaphoreType.DMA((2,))],
        [state, radius, cells, fluid_velocity],
        hbm=(2, 3),
        flops=1 << 25,
    )
    state, springs, *out = call(
        bind(middle_kernel, plan, sizes),
        [state_shape, spring_shape] + sends([f + e for f, e in zip(faces, extra)]),
        step_scratch,
        [state, radius, spread, inner, springs, partners, gas, pressure] + first_halos,
        flops=1 << 25,
    )
    halos = exchange(out, sizes)
    spread, inner = call(
        bind(inner_kernel, plan, False), [spread_shape, parts_shape], own_scratch,
        [state, radius], flops=1 << 25
    )
    width = 10 + 4 * hist
    padded = (width + 7) // 8 * 8
    places, speeds, turns, springs, state, *out = call(
        bind(last_kernel, plan, sizes),
        [three, three, three, spring_shape, state_shape] + sends([padded] * 3),
        step_scratch,
        [state, radius, spread, inner, springs, partners, gas, leaving] + halos,
        flops=1 << 25,
    )
    arrivals = exchange(out, sizes)
    force, new_pressure = call(
        bind(deposit_kernel, plan, sizes),
        [((3, nx, ny, nz), f32), ((nx, ny, nz), f32)],
        [
            vm(3, nx, ny, nz),
            vm(nx, ny, nz),
            pltpu.SemaphoreType.DMA((4 * plan.dims[0],)),
        ],
        [state, radius, cells, gas, pressure, pressure_source] + halos,
        outs_hbm=True,
        flops=1 << 25,
    )
    arrived, arrived_partners = call(
        bind(arrive_kernel, sizes),
        [((10 + 3 * hist, 6, 1, slots), f32), ((6, hist, slots), jnp.int32)],
        [],
        arrivals,
        flops=1 << 20,
    )
    wide = lambda a: a.reshape(a.shape[:-2] + radii.shape)
    return (
        wide(places),
        wide(speeds),
        wide(turns),
        wide(springs),
        force,
        new_pressure,
        arrived.reshape(1, 1, 1, 10 + 3 * hist, 6, slots),
        jnp.transpose(arrived_partners, (1, 0, 2))[None, None, None],
    )


def solution(mesh):
    sizes = tuple(mesh.shape[a] for a in AXES)
    return jax.shard_map(
        functools.partial(body, sizes),
        mesh=mesh,
        in_specs=(
            P(None, "gx", "gy", "gz", None),
            P(None, "gx", "gy", "gz", None),
            P(None, "gx", "gy", "gz", None),
            P("gx", "gy", "gz", None),
            P("gx", "gy", "gz"),
            P(None, None, "gx", "gy", "gz", None),
            P(None, "gx", "gy", "gz", None),
            P("gx", "gy", "gz", None),
            P("gx", "gy", "gz", None, None),
            P(None, "gx", "gy", "gz"),
            P("gx", "gy", "gz"),
            P("gx", "gy", "gz"),
        ),
        out_specs=(
            P(None, "gx", "gy", "gz", None),
            P(None, "gx", "gy", "gz", None),
            P(None, "gx", "gy", "gz", None),
            P(None, None, "gx", "gy", "gz", None),
            P(None, "gx", "gy", "gz"),
            P("gx", "gy", "gz"),
            P("gx", "gy", "gz", None, None, None),
            P("gx", "gy", "gz", None, None, None),
        ),
        check_vma=False,
    )
```

```python
import functools
import math

import jax
import jax.numpy as jnp
from jax import lax
from jax.experimental import pallas as pl
from jax.experimental.pallas import tpu as pltpu
from jax.sharding import PartitionSpec as P

SUBSTEPS = 2

normal_stiff = 100.0
normal_damp = 2.0
shear_stiff = 30.0
friction = 0.5
time_step = 0.05
drag_coeff = 0.8
gravity = 1.0
soft_length = 0.05
force_floor = 0.5
volume_coeff = 100.0
neighbours = ((0, 0, 0), (-1, 0, 0), (1, 0, 0), (0, -1, 0), (0, 1, 0), (0, 0, -1), (0, 0, 1))
AXES = ("gx", "gy", "gz")
FIELDS = 10
DEAD = -8.0
TINY = 1e-30
f32 = jnp.float32


class Plan:
    def __init__(self, shape):
        self.dims = shape
        self.count = shape[0] * shape[1] * shape[2]
        self.strides = (shape[1] * shape[2], shape[2], 1)

    def index(self, place):
        return (place[0] * self.dims[1] + place[1]) * self.dims[2] + place[2]

    def places(self):
        d = self.dims
        return [(a, b, c) for a in range(d[0]) for b in range(d[1]) for c in range(d[2])]

    def face(self, axis, side):
        edge = self.dims[axis] - 1 if side > 0 else 0
        return [self.index(p) for p in self.places() if p[axis] == edge]

    def neighbour(self, place, number):
        move = neighbours[number]
        other = tuple(p + m for p, m in zip(place, move))
        if all(0 <= o < d for o, d in zip(other, self.dims)):
            return True, self.index(other)
        axis = (number - 1) // 2
        across = [o for k, o in enumerate(place) if k != axis]
        width = [d for k, d in enumerate(self.dims) if k != axis][1]
        return False, across[0] * width + across[1]


def rolls(axis, sizes):
    size = sizes[AXES.index(axis)]
    if is_ring(axis, size):
        return [
            (axis, [(i, (i + 1) % size) for i in range(size)]),
            (axis, [((i + 1) % size, i) for i in range(size)]),
        ]

    def swaps(start):
        pairs = []
        for i in range(start, size - 1, 2):
            pairs += [(i, i + 1), (i + 1, i)]
        return pairs

    out = [(axis, swaps(0))]
    if size > 2:
        pairs = swaps(1)
        inside = [i for i, _ in pairs]
        across = sizes[0]
        if axis != "gx" and across % 2 == 0:
            joint = []
            for x in range(across):
                joint += [(x * size + i, x * size + j) for i, j in pairs]
                joint += [(x * size + i, (x ^ 1) * size + i) for i in range(size) if i not in inside]
            out.append((("gx", axis), joint))
        else:
            out.append((axis, pairs))
    return out


def is_ring(axis, size):
    return axis == "gx" and size > 2


def ordered_send(axis, size, low, high):
    if is_ring(axis, size):
        return [high, low]
    even = lax.axis_index(axis) % 2 == 0
    first = jnp.where(even, high, low)
    if size == 2:
        return [first]
    return [first, jnp.where(even, low, high)]


def ordered_receive(axis, size, blocks):
    if is_ring(axis, size):
        return blocks[0], blocks[1]
    if size == 2:
        return blocks[0], blocks[0]
    even = lax.axis_index(axis) % 2 == 0
    return jnp.where(even, blocks[1], blocks[0]), jnp.where(even, blocks[0], blocks[1])


def at_end(axis, size, side):
    edge = size - 1 if side > 0 else 0
    return lax.axis_index(axis) == edge


START_ORDER = (1, 0, 3, 2, 4)


def start_order(sizes):
    count = send_count(sizes)
    return START_ORDER if count == len(START_ORDER) else tuple(range(count))


def exchange(blocks, sizes):
    routes = [route for axis in AXES for route in rolls(axis, sizes)]
    routes = [routes[k] for k in start_order(sizes)]
    return [lax.ppermute(block, axes, pairs) for block, (axes, pairs) in zip(blocks, routes)]


def per_axis(refs, sizes):
    sorted_refs = [None] * len(refs)
    for ref, k in zip(refs, start_order(sizes)):
        sorted_refs[k] = ref
    out = []
    k = 0
    for axis in AXES:
        n = len(rolls(axis, sizes))
        out.append(sorted_refs[k : k + n])
        k += n
    return out


def send_count(sizes):
    return sum(len(rolls(a, sizes)) for a in AXES)


def put_faces(plan, sizes, state, sends):
    bins = plan.count
    sub = lax.broadcasted_iota(jnp.int32, state.shape[1:], 0)
    for axis, refs in enumerate(per_axis(sends, sizes)):
        stride, dim = plan.strides[axis], plan.dims[axis]
        level = sub // stride % dim
        for g in range(FIELDS // 2):
            one, two = state[2 * g], state[2 * g + 1]
            low = jnp.where(level == 0, one, pltpu.roll(two, stride % bins, 0))
            high = jnp.where(level == dim - 1, one, pltpu.roll(two, -stride % bins, 0))
            for ref, block in zip(refs, ordered_send(AXES[axis], sizes[axis], low, high)):
                ref[g * bins : (g + 1) * bins, :] = block


def pack_kernel(plan, sizes, pos, vel, spin, rad, counts_hbm, *refs):
    state, radius = refs[:2]
    sends = refs[2:-2]
    counts, sems = refs[-2:]
    copies = [
        pltpu.make_async_copy(rad, radius, sems.at[0]),
        pltpu.make_async_copy(pos, state.at[0:3], sems.at[1]),
        pltpu.make_async_copy(vel, state.at[3:6], sems.at[2]),
        pltpu.make_async_copy(spin, state.at[6:9], sems.at[3]),
        pltpu.make_async_copy(counts_hbm, counts, sems.at[4]),
    ]
    for copy in copies:
        copy.start()
    slots = rad.shape[-1]
    lane = lax.broadcasted_iota(jnp.int32, (1, slots), 1)
    places = plan.places()
    for copy in copies:
        copy.wait()
    for b in range(plan.count):
        x, y, z = places[b]
        live = lane < counts[x, y : y + 1, z : z + 1]
        state[9, b : b + 1, :] = jnp.where(live, radius[b : b + 1, :], DEAD)
    put_faces(plan, sizes, state, sends)


def put_pressure(plan, sizes, lanes, pressure, sends):
    nx, ny, nz = pressure.shape
    chunks = nz // lanes
    split = per_axis(sends, sizes)
    base = FIELDS // 2 * plan.count
    for ref, block in zip(
        split[0], ordered_send("gx", sizes[0], pressure[0], pressure[nx - 1])
    ):
        for c in range(chunks):
            ref[base + c * ny : base + (c + 1) * ny, :] = block[:, c * lanes : (c + 1) * lanes]
    base = FIELDS // 2 * plan.count
    for ref, block in zip(
        split[1], ordered_send("gy", sizes[1], pressure[:, 0, :], pressure[:, ny - 1, :])
    ):
        for c in range(chunks):
            ref[base + c * nx : base + (c + 1) * nx, :] = block[:, c * lanes : (c + 1) * lanes]
    base = FIELDS // 2 * plan.count
    wide = lax.broadcasted_iota(jnp.int32, (ny, lanes), 1)
    low = jnp.zeros((ny, lanes), f32)
    high = jnp.zeros((ny, lanes), f32)
    for x in range(nx):
        low = jnp.where(wide == x, jnp.broadcast_to(pressure[x, :, 0:1], (ny, lanes)), low)
        high = jnp.where(
            wide == x, jnp.broadcast_to(pressure[x, :, nz - 1 : nz], (ny, lanes)), high
        )
    for ref, block in zip(split[2], ordered_send("gz", sizes[2], low, high)):
        ref[base : base + ny, :] = block


def pair_rows(state, radius, mine):
    scale = normal_damp / normal_stiff
    for k in range(3):
        mine[:, k, :] = state[k]
        mine[:, 3 + k, :] = state[3 + k] * scale
    mine[:, 6, :] = radius[...]
    mine[:, 7, :] = radius[...]


def spread_rows(mine, spread):
    bins, fields, slots = mine.shape
    part = lax.broadcasted_iota(jnp.int32, (3 * fields, 7 * slots), 0) % fields
    block = lax.broadcasted_iota(jnp.int32, (3 * fields, 7 * slots), 1) // slots
    ones = (part == block).astype(jnp.bfloat16)
    for b in range(bins):
        rows = mine[b]
        top = rows.astype(jnp.bfloat16).astype(f32)
        left = rows - top
        mid = left.astype(jnp.bfloat16).astype(f32)
        parts = jnp.concatenate([top, mid, left - mid], axis=0).astype(jnp.bfloat16)
        wide = lax.dot_general(
            parts, ones, (((0,), (0,)), ((), ())), preferred_element_type=f32
        )
        for f in range(7):
            spread[b, f] = wide[:, f * slots : (f + 1) * slots]


def list_pairs(plan, entries, packed, table):
    slots = packed.shape[-1]
    lane = lax.broadcasted_iota(jnp.int32, (8, slots), 1)
    field = lax.broadcasted_iota(jnp.int32, (8, slots), 0)
    empty = jnp.where(field == 6, DEAD, 0.0)
    jobs = jnp.int32(0)
    for b in range(plan.count):
        start = jobs
        at = None
        for rows, count, move in entries[b]:
            value = rows
            for k in range(3):
                if move[k]:
                    value = value + jnp.where(field == k, float(move[k]), 0.0)
            if at is None:
                packed[start] = jnp.where(lane < count, value, empty)
                packed[start + 1] = empty
                at = count
                continue
            shift = at % slots
            job = start + at // slots
            moved = pltpu.roll(value, shift, 1)
            packed[job] = jnp.where(
                (lane >= shift) & (lane < shift + count), moved, packed[job]
            )
            packed[job + 1] = jnp.where(lane < shift + count - slots, moved, empty)
            at = at + count
        jobs = start + (at + slots - 1) // slots
        for q in range(len(entries[b])):
            table[start + q] = b
    return jobs


def run_pairs(jobs, spread, packed, table, parts):
    slots = packed.shape[-1]

    def job(t, carry):
        b = table[t]
        their = [jnp.broadcast_to(packed[t, f : f + 1, :], (8, slots)) for f in range(7)]
        for tile in range(slots // 8):
            rows = slice(tile * 8, tile * 8 + 8)
            own = [spread[b, f, rows, :] for f in range(7)]
            sep = [own[k] - their[k] for k in range(3)]
            square = sep[0] * sep[0] + (sep[1] * sep[1] + (sep[2] * sep[2] + soft_length**2))
            inverse = lax.rsqrt(square)
            over = (own[6] + their[6]) - square * inverse
            positive = jnp.maximum(over, 0.0)
            root = positive * lax.rsqrt(jnp.maximum(over, TINY))
            dot = (own[3] - their[3]) * sep[0]
            dot = dot + (own[4] - their[4]) * sep[1]
            dot = dot + (own[5] - their[5]) * sep[2]
            weight = (positive - dot * inverse) * (root * inverse)
            for k in range(3):
                parts[b, k, rows, :] = parts[b, k, rows, :] + weight * sep[k]
        return carry

    lax.fori_loop(0, jobs, job, 0)


def inner_kernel(plan, with_fluid, *refs):
    if with_fluid:
        (state, radius, cells_hbm, fluid_hbm, spread, parts, gas, cells, mine, packed,
         table, fluid, sems) = refs
        fetches = [
            pltpu.make_async_copy(cells_hbm, cells, sems.at[0]),
            pltpu.make_async_copy(fluid_hbm, fluid, sems.at[1]),
        ]
        for fetch in fetches:
            fetch.start()
    else:
        state, radius, spread, parts, mine, packed, table = refs
    parts[...] = jnp.zeros_like(parts)
    pair_rows(state, radius, mine)
    spread_rows(mine, spread)
    records = []
    for b in range(plan.count):
        rows = mine[b]
        field = lax.broadcasted_iota(jnp.int32, rows.shape, 0)
        records.append(jnp.where(field == 6, state[9, b : b + 1, :], rows))
    filled = jnp.sum(jnp.where(state[9] > 0.0, 1, 0), axis=1, keepdims=True)
    entries = []
    for place in plan.places():
        entry = []
        for n in range(7):
            own, other = plan.neighbour(place, n)
            if own:
                entry.append((records[other], filled[other, 0], neighbours[n]))
        entries.append(entry)
    jobs = list_pairs(plan, entries, packed, table)
    run_pairs(jobs, spread, packed, table, parts)
    if not with_fluid:
        return
    for fetch in fetches:
        fetch.wait()
    slots = radius.shape[-1]
    span = [s // d for s, d in zip(fluid.shape[1:], plan.dims)]
    sub = lax.broadcasted_iota(jnp.int32, (8, slots), 0)
    for place in plan.places():
        b = plan.index(place)
        cell = cells[b : b + 1, :]
        column = jnp.broadcast_to(cell % span[2], (8, slots))
        row = jnp.broadcast_to(cell // span[2], (8, slots)) - sub
        sums_c = [jnp.zeros((8, slots), f32) for c in range(3)]
        for a in range(span[0]):
            for h in range(span[1] // 8):
                hit = row == a * span[1] + h * 8
                y0 = place[1] * span[1] + h * 8
                z0 = place[2] * span[2]
                for c in range(3):
                    block = fluid[c, place[0] * span[0] + a, y0 : y0 + 8, z0 : z0 + span[2]]
                    got = jnp.take_along_axis(block, column, axis=1)
                    sums_c[c] = jnp.where(hit, got, sums_c[c])
        for c in range(3):
            gas[c, b : b + 1, :] = jnp.sum(sums_c[c], axis=0, keepdims=True)


def step_core(plan, sizes, state, radius, spread, inner, springs, partners, gas, halos, out,
              new_springs, around, beside, packed, table, parts):
    scale = normal_damp / normal_stiff
    places = plan.places()
    slots = radius.shape[-1]
    split = per_axis(halos, sizes)
    around[0] = state[...]
    sub = lax.broadcasted_iota(jnp.int32, (plan.count, slots), 0)
    inner_count = [plan.dims[1] * plan.dims[2], plan.dims[2], 1]
    entries = [[] for _ in places]
    parts[...] = inner[...]
    bins = plan.count
    for axis in range(3):
        stride = inner_count[axis]
        dim = plan.dims[axis]
        level = sub // stride % dim
        for f in range(FIELDS):
            rows = slice(f // 2 * bins, (f // 2 + 1) * bins)
            far = (dim - 1 - f % 2) * stride
            got = ordered_receive(AXES[axis], sizes[axis], [ref[rows, :] for ref in split[axis]])
            for side in (-1, 1):
                n = 2 * axis + (1 if side < 0 else 2)
                edge = dim - 1 if side > 0 else 0
                own = pltpu.roll(state[f], -side * stride % bins, 0)
                other = pltpu.roll(got[1 if side > 0 else 0], side * far % bins, 0)
                value = jnp.where(level == edge, other, own)
                if f == 9:
                    gone = at_end(AXES[axis], sizes[axis], side)
                    value = jnp.where(((level == edge) & gone) | (value <= 0.0), DEAD, value)
                    beside[n, :, 6, :] = value
                    beside[n, :, 7, :] = value
                    filled = jnp.sum(jnp.where(value > 0.0, 1, 0), axis=1, keepdims=True)
                    for place in places:
                        if not plan.neighbour(place, n)[0]:
                            b = plan.index(place)
                            entries[b].append((n, filled[b, 0]))
                elif f < 3:
                    beside[n, :, f, :] = value + float(neighbours[n][f])
                elif f < 6:
                    beside[n, :, f, :] = value * scale
                around[n, f] = value
    entries = [
        [(beside[n, b], count, (0, 0, 0)) for n, count in entries[b]] for b in range(bins)
    ]
    jobs = list_pairs(plan, entries, packed, table)
    run_pairs(jobs, spread, packed, table, parts)
    normal = []
    for k in range(3):
        sums = [
            jnp.sum(jnp.transpose(parts[b, k], (1, 0)), axis=0, keepdims=True)
            for b in range(plan.count)
        ]
        normal.append(jnp.concatenate(sums, axis=0) * normal_stiff)
    place_i = [state[k] for k in range(3)]
    speed_i = [state[3 + k] for k in range(3)]
    turn_i = [state[6 + k] for k in range(3)]
    rad_i = radius[...]
    shear_sum = [jnp.zeros_like(rad_i) for k in range(3)]
    twist = [jnp.zeros_like(rad_i) for k in range(3)]
    for h in range(partners.shape[0]):
        code = partners[h]
        valid = code >= 0
        code = jnp.maximum(code, 0)
        which = code // slots
        member = code % slots
        picked = []
        for f in range(FIELDS):
            value = jnp.take_along_axis(around[0, f], member, axis=1)
            for n in range(1, 7):
                got = jnp.take_along_axis(around[n, f], member, axis=1)
                value = jnp.where(which == n, got, value)
            picked.append(value)
        alive = valid & (picked[9] > 0.0)
        sep = []
        for k in range(3):
            shift = jnp.where(which == 2 + 2 * k, 1.0, jnp.where(which == 1 + 2 * k, -1.0, 0.0))
            sep.append(place_i[k] - picked[k] - shift)
        distance = jnp.sqrt(sep[0] * sep[0] + sep[1] * sep[1] + sep[2] * sep[2] + soft_length**2)
        unit = [s / distance for s in sep]
        over = jnp.maximum(rad_i + picked[9] - distance, 0.0)
        root = jnp.sqrt(over)
        rel = [speed_i[k] - picked[3 + k] for k in range(3)]
        approach = rel[0] * unit[0] + rel[1] * unit[1] + rel[2] * unit[2]
        pressing = normal_stiff * over * root - normal_damp * root * approach
        lever = [rad_i * turn_i[k] + picked[9] * picked[6 + k] for k in range(3)]
        contact = [
            rel[k]
            - (
                lever[(k + 1) % 3] * unit[(k + 2) % 3]
                - lever[(k + 2) % 3] * unit[(k + 1) % 3]
            )
            for k in range(3)
        ]
        along = contact[0] * unit[0] + contact[1] * unit[1] + contact[2] * unit[2]
        old = [springs[k, h] for k in range(3)]
        old_along = old[0] * unit[0] + old[1] * unit[1] + old[2] * unit[2]
        stretched = [
            old[k] - old_along * unit[k] + time_step * (contact[k] - along * unit[k])
            for k in range(3)
        ]
        length = jnp.sqrt(
            stretched[0] * stretched[0] + stretched[1] * stretched[1] + stretched[2] * stretched[2]
        )
        limit = jnp.minimum(
            1.0, friction * jnp.abs(pressing) / jnp.maximum(shear_stiff * length, force_floor)
        )
        limit = jnp.where(alive, limit, 0.0)
        fresh = [limit * stretched[k] for k in range(3)]
        for k in range(3):
            new_springs[k, h] = fresh[k]
            shear_sum[k] = shear_sum[k] - shear_stiff * fresh[k]
            twist[k] = twist[k] - shear_stiff * (
                fresh[(k + 1) % 3] * unit[(k + 2) % 3] - fresh[(k + 2) % 3] * unit[(k + 1) % 3]
            )
    safe = jnp.where(rad_i > 0.0, rad_i, 1.0)
    ratio = safe / 0.1
    mass = ratio * ratio * ratio
    inertia = 0.4 * mass * safe * safe
    for k in range(3):
        force = normal[k] + shear_sum[k] + drag_coeff * (gas[k] - speed_i[k])
        lift = gravity if k == 2 else 0.0
        speed = speed_i[k] + time_step * (force / mass - lift)
        out[k] = place_i[k] + time_step * speed
        out[3 + k] = speed
        out[6 + k] = turn_i[k] + time_step * (rad_i * twist[k]) / inertia
    out[9] = state[9]


def middle_kernel(plan, sizes, *refs):
    n = send_count(sizes)
    state, radius, spread, inner, springs, partners, gas, pressure = refs[:8]
    halos = refs[8 : 8 + n]
    out, new_springs = refs[8 + n : 10 + n]
    sends = refs[10 + n : 10 + 2 * n]
    scratch = refs[10 + 2 * n :]
    put_pressure(plan, sizes, radius.shape[-1], pressure, sends)
    step_core(plan, sizes, state, radius, spread, inner, springs, partners, gas, halos, out,
              new_springs, *scratch)
    put_faces(plan, sizes, out, sends)


def last_kernel(plan, sizes, *refs):
    n = send_count(sizes)
    state, radius, spread, inner, springs, partners, gas, departures = refs[:8]
    halos = refs[8 : 8 + n]
    places, speeds, turns, new_springs, out = refs[8 + n : 13 + n]
    sends = refs[13 + n : 13 + 2 * n]
    scratch = refs[13 + 2 * n :]
    step_core(plan, sizes, state, radius, spread, inner, springs, partners, gas, halos, out,
              new_springs, *scratch)
    places[...] = out[0:3]
    speeds[...] = out[3:6]
    turns[...] = out[6:9]
    slots = radius.shape[-1]
    hist = partners.shape[0]
    count = plan.count
    sub = lax.broadcasted_iota(jnp.int32, (count, slots), 0)
    values = [out[f] for f in range(9)] + [radius[...]]
    values += [new_springs[k, h] for k in range(3) for h in range(hist)]
    values += [(partners[h] + 1).astype(f32) for h in range(hist)]
    width = len(values)
    picks = [[], [], [], [], [], []]
    for d in range(6):
        leaving = jnp.broadcast_to(departures[d : d + 1, :], (count, slots))
        hit = (leaving // slots == sub) & (leaving >= 0)
        member = jnp.maximum(leaving, 0) % slots
        for v in values:
            got = jnp.where(hit, jnp.take_along_axis(v, member, axis=1), 0.0)
            picks[d].append(jnp.sum(got, axis=0, keepdims=True))
    split = per_axis(sends, sizes)
    for axis in range(3):
        for f in range(width):
            blocks = ordered_send(
                AXES[axis], sizes[axis], picks[2 * axis][f], picks[2 * axis + 1][f]
            )
            for ref, block in zip(split[axis], blocks):
                ref[f : f + 1, :] = block


def deposit_kernel(plan, sizes, *refs):
    n = send_count(sizes)
    state, radius, cells, gas, pressure, source = refs[:6]
    halos = refs[6 : 6 + n]
    force_out, pressure_out, force, new_pressure, sems = refs[6 + n :]
    copies = []

    def send(source, target):
        copies.append(pltpu.make_async_copy(source, target, sems.at[len(copies)]))
        copies[-1].start()

    slots = radius.shape[-1]
    nx, ny, nz = pressure.shape
    lanes = slots
    chunks = nz // lanes
    span = [s // d for s, d in zip(pressure.shape, plan.dims)]
    rows = span[0] * span[1]
    high_row = lax.broadcasted_iota(jnp.int32, (rows, slots), 0)
    column_row = lax.broadcasted_iota(jnp.int32, (span[2], slots), 0)
    def deposit(place):
        b = plan.index(place)
        cell = cells[b : b + 1, :]
        live = state[9, b : b + 1, :] > 0.0
        rad = radius[b : b + 1, :]
        values = [
            jnp.where(live, drag_coeff * (state[3 + c, b : b + 1, :] - gas[c, b : b + 1, :]), 0.0)
            for c in range(3)
        ]
        values.append(jnp.where(live, 4.0 / 3.0 * math.pi * rad * rad * rad, 0.0))
        at_row = high_row == cell // span[2]
        at_column = (column_row == cell % span[2]).astype(jnp.bfloat16)
        halves = []
        for v in values:
            top = v.astype(jnp.bfloat16).astype(f32)
            left = v - top
            halves.append(
                jnp.concatenate(
                    [jnp.where(at_row, part, 0.0).astype(jnp.bfloat16) for part in (top, left)],
                    axis=1,
                )
            )
        left = jnp.concatenate(halves, axis=0)
        right = jnp.concatenate([at_column] * 2, axis=1)
        got = lax.dot_general(
            left, right, (((1,), (1,)), ((), ())), preferred_element_type=f32
        )
        x0, y0, z0 = (p * s for p, s in zip(place, span))
        block = (slice(x0, x0 + span[0]), slice(y0, y0 + span[1]), slice(z0, z0 + span[2]))
        pieces = [got[c * rows : (c + 1) * rows].reshape(span) for c in range(4)]
        for c in range(3):
            force[(c,) + block] = pieces[c]
        new_pressure[block] = volume_coeff * pieces[3] + pieces[2]
    split = per_axis(halos, sizes)
    dead = [
        [at_end(AXES[axis], sizes[axis], side) for side in (-1, 1)] for axis in range(3)
    ]
    base = FIELDS // 2 * plan.count
    slabs = []
    for ref in split[0]:
        slabs.append(
            jnp.concatenate(
                [ref[base + c * ny : base + (c + 1) * ny, :] for c in range(chunks)], axis=1
            )
        )
    x_ends = ordered_receive("gx", sizes[0], slabs)
    x_ends = [jnp.where(dead[0][s], 0.0, x_ends[s]) for s in (0, 1)]
    base = FIELDS // 2 * plan.count
    slabs = []
    for ref in split[1]:
        slabs.append(
            jnp.concatenate(
                [ref[base + c * nx : base + (c + 1) * nx, :] for c in range(chunks)], axis=1
            )
        )
    y_ends = ordered_receive("gy", sizes[1], slabs)
    y_ends = [jnp.where(dead[1][s], 0.0, y_ends[s]) for s in (0, 1)]
    base = FIELDS // 2 * plan.count
    z_ends = ordered_receive("gz", sizes[2], [ref[base : base + ny, :] for ref in split[2]])
    z_ends = [jnp.where(dead[2][s], 0.0, z_ends[s]) for s in (0, 1)]
    row = lax.broadcasted_iota(jnp.int32, (ny, nz), 0)
    column = lax.broadcasted_iota(jnp.int32, (ny, nz), 1)
    def sweep(x):
        here = pressure[x]
        total = pressure[x - 1] if x > 0 else x_ends[0]
        total = total + (pressure[x + 1] if x < nx - 1 else x_ends[1])
        total = total + jnp.where(row == 0, y_ends[0][x : x + 1, :], pltpu.roll(here, 1, 0))
        total = total + jnp.where(
            row == ny - 1, y_ends[1][x : x + 1, :], pltpu.roll(here, ny - 1, 0)
        )
        total = total + jnp.where(column == 0, z_ends[0][:, x : x + 1], pltpu.roll(here, 1, 1))
        total = total + jnp.where(
            column == nz - 1, z_ends[1][:, x : x + 1], pltpu.roll(here, nz - 1, 1)
        )
        new_pressure[x] = (total + (source[x] + new_pressure[x])) * (1.0 / 6.0)

    layers = plan.dims[0]
    for layer in range(layers + 1):
        if layer < layers:
            for place in plan.places():
                if place[0] == layer:
                    deposit(place)
        if layer > 0:
            for x in range((layer - 1) * span[0], layer * span[0]):
                sweep(x)
        if layer < layers:
            part = slice(layer * span[0], (layer + 1) * span[0])
            for c in range(3):
                send(force.at[c, part], force_out.at[c, part])
        if layer > 0:
            part = slice((layer - 1) * span[0], layer * span[0])
            send(new_pressure.at[part], pressure_out.at[part])
    for copy in copies:
        copy.wait()


def arrive_kernel(sizes, *refs):
    n = send_count(sizes)
    halos = refs[:n]
    state, codes = refs[n:]
    split = per_axis(halos, sizes)
    width = state.shape[0]
    hist = codes.shape[1]
    for axis in range(3):
        got = [ref[0 : width + hist, :] for ref in split[axis]]
        before, after = ordered_receive(AXES[axis], sizes[axis], got)
        after = jnp.where(at_end(AXES[axis], sizes[axis], 1), 0.0, after)
        before = jnp.where(at_end(AXES[axis], sizes[axis], -1), 0.0, before)
        for d, block in ((2 * axis, after), (2 * axis + 1, before)):
            state[:, d, 0, :] = block[0:width]
            codes[d] = block[width : width + hist].astype(jnp.int32) - 1


def call(kernel, outs, scratch, args, hbm=(), flops=0, outs_hbm=False):
    specs = []
    args = [
        pltpu.with_memory_space_constraint(a, pltpu.HBM) if k in hbm else a
        for k, a in enumerate(args)
    ]
    for k in range(len(args)):
        space = pltpu.HBM if k in hbm else pltpu.VMEM
        specs.append(pl.BlockSpec(memory_space=space))
    return pl.pallas_call(
        kernel,
        out_shape=[jax.ShapeDtypeStruct(s, d) for s, d in outs],
        in_specs=specs,
        out_specs=[pl.BlockSpec(memory_space=pltpu.HBM if outs_hbm else pltpu.VMEM)] * len(outs),
        scratch_shapes=scratch,
        compiler_params=pltpu.CompilerParams(vmem_limit_bytes=32 * 1024 * 1024),
        cost_estimate=pl.CostEstimate(flops=flops, bytes_accessed=1 << 20, transcendentals=0),
    )(*args)


def body(sizes, positions, velocities, spins, radii, counts, springs, partners, cells, departures,
         fluid_velocity, pressure, pressure_source):
    plan = Plan(radii.shape[:3])
    count = plan.count
    slots = radii.shape[3]
    hist = partners.shape[0]
    nx, ny, nz = pressure.shape
    chunks = nz // slots
    flat = lambda a: a.reshape(a.shape[:-4] + (count, slots))
    pos, vel, spin = flat(positions), flat(velocities), flat(spins)
    radius = radii.reshape(count, slots)
    springs = springs.reshape(3, hist, count, slots)
    partners = partners.reshape(hist, count, slots)
    cells = cells.reshape(count, slots)
    leaving = departures.reshape(6, slots)

    faces = [FIELDS // 2 * count] * 3
    extra = [chunks * ny, chunks * nx, ny]
    vm = lambda *s: pltpu.VMEM(s, f32)

    def sends(rows):
        out = []
        for a in range(3):
            for _ in rolls(AXES[a], sizes):
                out.append(((rows[a], slots), f32))
        return [out[k] for k in start_order(sizes)]

    inside = [sum(plan.neighbour(p, n)[0] for n in range(7)) for p in plan.places()]

    def pair_scratch(jobs):
        return [vm(jobs + 2, 8, slots), pltpu.SMEM((jobs + 8,), jnp.int32)]

    own_scratch = [vm(count, 8, slots)] + pair_scratch(sum(inside))
    spread_shape = ((count, 7, slots, slots), f32)
    parts_shape = ((count, 3, slots, slots), f32)
    step_scratch = [vm(7, FIELDS, count, slots), vm(7, count, 8, slots)] + pair_scratch(7 * count - sum(inside))
    step_scratch.append(vm(count, 3, slots, slots))
    state_shape = ((FIELDS, count, slots), f32)
    three = ((3, count, slots), f32)
    spring_shape = ((3, hist, count, slots), f32)
    bind = functools.partial

    state, radius, *out = call(
        bind(pack_kernel, plan, sizes),
        [state_shape, ((count, slots), f32)] + sends(faces),
        [
            pltpu.VMEM(counts.shape, jnp.int32),
            pltpu.SemaphoreType.DMA((5,)),
        ],
        [pos, vel, spin, radius, counts],
        hbm=(0, 1, 2, 3, 4),
        flops=1 << 20,
    )
    first_halos = exchange(out, sizes)
    spread, inner, gas, cells = call(
        bind(inner_kernel, plan, True),
        [spread_shape, parts_shape, three, ((count, slots), jnp.int32)],
        own_scratch + [vm(3, nx, ny, nz), pltpu.SemaphoreType.DMA((2,))],
        [state, radius, cells, fluid_velocity],
        hbm=(2, 3),
        flops=1 << 25,
    )
    state, springs, *out = call(
        bind(middle_kernel, plan, sizes),
        [state_shape, spring_shape] + sends([f + e for f, e in zip(faces, extra)]),
        step_scratch,
        [state, radius, spread, inner, springs, partners, gas, pressure] + first_halos,
        flops=1 << 25,
    )
    halos = exchange(out, sizes)
    spread, inner = call(
        bind(inner_kernel, plan, False), [spread_shape, parts_shape], own_scratch,
        [state, radius], flops=1 << 25
    )
    width = 10 + 4 * hist
    padded = (width + 7) // 8 * 8
    places, speeds, turns, springs, state, *out = call(
        bind(last_kernel, plan, sizes),
        [three, three, three, spring_shape, state_shape] + sends([padded] * 3),
        step_scratch,
        [state, radius, spread, inner, springs, partners, gas, leaving] + halos,
        flops=1 << 25,
    )
    arrivals = exchange(out, sizes)
    force, new_pressure = call(
        bind(deposit_kernel, plan, sizes),
        [((3, nx, ny, nz), f32), ((nx, ny, nz), f32)],
        [
            vm(3, nx, ny, nz),
            vm(nx, ny, nz),
            pltpu.SemaphoreType.DMA((4 * plan.dims[0],)),
        ],
        [state, radius, cells, gas, pressure, pressure_source] + halos,
        outs_hbm=True,
        flops=1 << 25,
    )
    arrived, arrived_partners = call(
        bind(arrive_kernel, sizes),
        [((10 + 3 * hist, 6, 1, slots), f32), ((6, hist, slots), jnp.int32)],
        [],
        arrivals,
        flops=1 << 20,
    )
    wide = lambda a: a.reshape(a.shape[:-2] + radii.shape)
    return (
        wide(places),
        wide(speeds),
        wide(turns),
        wide(springs),
        force,
        new_pressure,
        arrived.reshape(1, 1, 1, 10 + 3 * hist, 6, slots),
        jnp.transpose(arrived_partners, (1, 0, 2))[None, None, None],
    )


def solution(mesh):
    sizes = tuple(mesh.shape[a] for a in AXES)
    return jax.shard_map(
        functools.partial(body, sizes),
        mesh=mesh,
        in_specs=(
            P(None, "gx", "gy", "gz", None),
            P(None, "gx", "gy", "gz", None),
            P(None, "gx", "gy", "gz", None),
            P("gx", "gy", "gz", None),
            P("gx", "gy", "gz"),
            P(None, None, "gx", "gy", "gz", None),
            P(None, "gx", "gy", "gz", None),
            P("gx", "gy", "gz", None),
            P("gx", "gy", "gz", None, None),
            P(None, "gx", "gy", "gz"),
            P("gx", "gy", "gz"),
            P("gx", "gy", "gz"),
        ),
        out_specs=(
            P(None, "gx", "gy", "gz", None),
            P(None, "gx", "gy", "gz", None),
            P(None, "gx", "gy", "gz", None),
            P(None, None, "gx", "gy", "gz", None),
            P(None, "gx", "gy", "gz"),
            P("gx", "gy", "gz"),
            P("gx", "gy", "gz", None, None, None),
            P("gx", "gy", "gz", None, None, None),
        ),
        check_vma=False,
    )
```

```python
import functools
import math

import jax
import jax.numpy as jnp
from jax import lax
from jax.experimental import pallas as pl
from jax.experimental.pallas import tpu as pltpu
from jax.sharding import PartitionSpec as P

SUBSTEPS = 2

normal_stiff = 100.0
normal_damp = 2.0
shear_stiff = 30.0
friction = 0.5
time_step = 0.05
drag_coeff = 0.8
gravity = 1.0
soft_length = 0.05
force_floor = 0.5
volume_coeff = 100.0
neighbours = ((0, 0, 0), (-1, 0, 0), (1, 0, 0), (0, -1, 0), (0, 1, 0), (0, 0, -1), (0, 0, 1))
AXES = ("gx", "gy", "gz")
FIELDS = 10
DEAD = -8.0
TINY = 1e-30
f32 = jnp.float32


class Plan:
    def __init__(self, shape):
        self.dims = shape
        self.count = shape[0] * shape[1] * shape[2]
        self.strides = (shape[1] * shape[2], shape[2], 1)

    def index(self, place):
        return (place[0] * self.dims[1] + place[1]) * self.dims[2] + place[2]

    def places(self):
        d = self.dims
        return [(a, b, c) for a in range(d[0]) for b in range(d[1]) for c in range(d[2])]

    def face(self, axis, side):
        edge = self.dims[axis] - 1 if side > 0 else 0
        return [self.index(p) for p in self.places() if p[axis] == edge]

    def neighbour(self, place, number):
        move = neighbours[number]
        other = tuple(p + m for p, m in zip(place, move))
        if all(0 <= o < d for o, d in zip(other, self.dims)):
            return True, self.index(other)
        axis = (number - 1) // 2
        across = [o for k, o in enumerate(place) if k != axis]
        width = [d for k, d in enumerate(self.dims) if k != axis][1]
        return False, across[0] * width + across[1]


def rolls(axis, sizes):
    size = sizes[AXES.index(axis)]
    if is_ring(axis, size):
        return [
            (axis, [(i, (i + 1) % size) for i in range(size)]),
            (axis, [((i + 1) % size, i) for i in range(size)]),
        ]

    def swaps(start):
        pairs = []
        for i in range(start, size - 1, 2):
            pairs += [(i, i + 1), (i + 1, i)]
        return pairs

    out = [(axis, swaps(0))]
    if size > 2:
        pairs = swaps(1)
        inside = [i for i, _ in pairs]
        across = sizes[0]
        if axis != "gx" and across % 2 == 0:
            joint = []
            for x in range(across):
                joint += [(x * size + i, x * size + j) for i, j in pairs]
                joint += [(x * size + i, (x ^ 1) * size + i) for i in range(size) if i not in inside]
            out.append((("gx", axis), joint))
        else:
            out.append((axis, pairs))
    return out


def is_ring(axis, size):
    return axis == "gx" and size > 2


def ordered_send(axis, size, low, high):
    if is_ring(axis, size):
        return [high, low]
    even = lax.axis_index(axis) % 2 == 0
    first = jnp.where(even, high, low)
    if size == 2:
        return [first]
    return [first, jnp.where(even, low, high)]


def ordered_receive(axis, size, blocks):
    if is_ring(axis, size):
        return blocks[0], blocks[1]
    if size == 2:
        return blocks[0], blocks[0]
    even = lax.axis_index(axis) % 2 == 0
    return jnp.where(even, blocks[1], blocks[0]), jnp.where(even, blocks[0], blocks[1])


def at_end(axis, size, side):
    edge = size - 1 if side > 0 else 0
    return lax.axis_index(axis) == edge


START_ORDER = (1, 0, 3, 4, 2)


def start_order(sizes):
    count = send_count(sizes)
    return START_ORDER if count == len(START_ORDER) else tuple(range(count))


def exchange(blocks, sizes):
    routes = [route for axis in AXES for route in rolls(axis, sizes)]
    routes = [routes[k] for k in start_order(sizes)]
    return [lax.ppermute(block, axes, pairs) for block, (axes, pairs) in zip(blocks, routes)]


def per_axis(refs, sizes):
    sorted_refs = [None] * len(refs)
    for ref, k in zip(refs, start_order(sizes)):
        sorted_refs[k] = ref
    out = []
    k = 0
    for axis in AXES:
        n = len(rolls(axis, sizes))
        out.append(sorted_refs[k : k + n])
        k += n
    return out


def send_count(sizes):
    return sum(len(rolls(a, sizes)) for a in AXES)


def put_faces(plan, sizes, state, sends):
    bins = plan.count
    sub = lax.broadcasted_iota(jnp.int32, state.shape[1:], 0)
    for axis, refs in enumerate(per_axis(sends, sizes)):
        stride, dim = plan.strides[axis], plan.dims[axis]
        level = sub // stride % dim
        for g in range(FIELDS // 2):
            one, two = state[2 * g], state[2 * g + 1]
            low = jnp.where(level == 0, one, pltpu.roll(two, stride % bins, 0))
            high = jnp.where(level == dim - 1, one, pltpu.roll(two, -stride % bins, 0))
            for ref, block in zip(refs, ordered_send(AXES[axis], sizes[axis], low, high)):
                ref[g * bins : (g + 1) * bins, :] = block


def pack_kernel(plan, sizes, pos, vel, spin, rad, counts_hbm, *refs):
    state, radius = refs[:2]
    sends = refs[2:-2]
    counts, sems = refs[-2:]
    copies = [
        pltpu.make_async_copy(rad, radius, sems.at[0]),
        pltpu.make_async_copy(pos, state.at[0:3], sems.at[1]),
        pltpu.make_async_copy(vel, state.at[3:6], sems.at[2]),
        pltpu.make_async_copy(spin, state.at[6:9], sems.at[3]),
        pltpu.make_async_copy(counts_hbm, counts, sems.at[4]),
    ]
    for copy in copies:
        copy.start()
    slots = rad.shape[-1]
    lane = lax.broadcasted_iota(jnp.int32, (1, slots), 1)
    places = plan.places()
    for copy in copies:
        copy.wait()
    for b in range(plan.count):
        x, y, z = places[b]
        live = lane < counts[x, y : y + 1, z : z + 1]
        state[9, b : b + 1, :] = jnp.where(live, radius[b : b + 1, :], DEAD)
    put_faces(plan, sizes, state, sends)


def put_pressure(plan, sizes, lanes, pressure, sends):
    nx, ny, nz = pressure.shape
    chunks = nz // lanes
    split = per_axis(sends, sizes)
    base = FIELDS // 2 * plan.count
    for ref, block in zip(
        split[0], ordered_send("gx", sizes[0], pressure[0], pressure[nx - 1])
    ):
        for c in range(chunks):
            ref[base + c * ny : base + (c + 1) * ny, :] = block[:, c * lanes : (c + 1) * lanes]
    base = FIELDS // 2 * plan.count
    for ref, block in zip(
        split[1], ordered_send("gy", sizes[1], pressure[:, 0, :], pressure[:, ny - 1, :])
    ):
        for c in range(chunks):
            ref[base + c * nx : base + (c + 1) * nx, :] = block[:, c * lanes : (c + 1) * lanes]
    base = FIELDS // 2 * plan.count
    wide = lax.broadcasted_iota(jnp.int32, (ny, lanes), 1)
    low = jnp.zeros((ny, lanes), f32)
    high = jnp.zeros((ny, lanes), f32)
    for x in range(nx):
        low = jnp.where(wide == x, jnp.broadcast_to(pressure[x, :, 0:1], (ny, lanes)), low)
        high = jnp.where(
            wide == x, jnp.broadcast_to(pressure[x, :, nz - 1 : nz], (ny, lanes)), high
        )
    for ref, block in zip(split[2], ordered_send("gz", sizes[2], low, high)):
        ref[base : base + ny, :] = block


def pair_rows(state, radius, mine):
    scale = normal_damp / normal_stiff
    for k in range(3):
        mine[:, k, :] = state[k]
        mine[:, 3 + k, :] = state[3 + k] * scale
    mine[:, 6, :] = radius[...]
    mine[:, 7, :] = radius[...]


def spread_rows(mine, spread):
    bins, fields, slots = mine.shape
    part = lax.broadcasted_iota(jnp.int32, (3 * fields, 7 * slots), 0) % fields
    block = lax.broadcasted_iota(jnp.int32, (3 * fields, 7 * slots), 1) // slots
    ones = (part == block).astype(jnp.bfloat16)
    for b in range(bins):
        rows = mine[b]
        top = rows.astype(jnp.bfloat16).astype(f32)
        left = rows - top
        mid = left.astype(jnp.bfloat16).astype(f32)
        parts = jnp.concatenate([top, mid, left - mid], axis=0).astype(jnp.bfloat16)
        wide = lax.dot_general(
            parts, ones, (((0,), (0,)), ((), ())), preferred_element_type=f32
        )
        for f in range(7):
            spread[b, f] = wide[:, f * slots : (f + 1) * slots]


def list_pairs(plan, entries, packed, table):
    slots = packed.shape[-1]
    lane = lax.broadcasted_iota(jnp.int32, (8, slots), 1)
    field = lax.broadcasted_iota(jnp.int32, (8, slots), 0)
    empty = jnp.where(field == 6, DEAD, 0.0)
    jobs = jnp.int32(0)
    for b in range(plan.count):
        start = jobs
        at = None
        for rows, count, move in entries[b]:
            value = rows
            for k in range(3):
                if move[k]:
                    value = value + jnp.where(field == k, float(move[k]), 0.0)
            if at is None:
                packed[start] = jnp.where(lane < count, value, empty)
                packed[start + 1] = empty
                at = count
                continue
            shift = at % slots
            job = start + at // slots
            moved = pltpu.roll(value, shift, 1)
            packed[job] = jnp.where(
                (lane >= shift) & (lane < shift + count), moved, packed[job]
            )
            packed[job + 1] = jnp.where(lane < shift + count - slots, moved, empty)
            at = at + count
        jobs = start + (at + slots - 1) // slots
        for q in range(len(entries[b])):
            table[start + q] = b
    return jobs


def run_pairs(jobs, spread, packed, table, parts):
    slots = packed.shape[-1]

    def job(t, carry):
        b = table[t]
        their = [jnp.broadcast_to(packed[t, f : f + 1, :], (8, slots)) for f in range(7)]
        for tile in range(slots // 8):
            rows = slice(tile * 8, tile * 8 + 8)
            own = [spread[b, f, rows, :] for f in range(7)]
            sep = [own[k] - their[k] for k in range(3)]
            square = sep[0] * sep[0] + (sep[1] * sep[1] + (sep[2] * sep[2] + soft_length**2))
            inverse = lax.rsqrt(square)
            over = (own[6] + their[6]) - square * inverse
            positive = jnp.maximum(over, 0.0)
            root = positive * lax.rsqrt(jnp.maximum(over, TINY))
            dot = (own[3] - their[3]) * sep[0]
            dot = dot + (own[4] - their[4]) * sep[1]
            dot = dot + (own[5] - their[5]) * sep[2]
            weight = (positive - dot * inverse) * (root * inverse)
            for k in range(3):
                parts[b, k, rows, :] = parts[b, k, rows, :] + weight * sep[k]
        return carry

    lax.fori_loop(0, jobs, job, 0)


def inner_kernel(plan, with_fluid, *refs):
    if with_fluid:
        (state, radius, cells_hbm, fluid_hbm, spread, parts, gas, cells, mine, packed,
         table, fluid, sems) = refs
        fetches = [
            pltpu.make_async_copy(cells_hbm, cells, sems.at[0]),
            pltpu.make_async_copy(fluid_hbm, fluid, sems.at[1]),
        ]
        for fetch in fetches:
            fetch.start()
    else:
        state, radius, spread, parts, mine, packed, table = refs
    parts[...] = jnp.zeros_like(parts)
    pair_rows(state, radius, mine)
    spread_rows(mine, spread)
    records = []
    for b in range(plan.count):
        rows = mine[b]
        field = lax.broadcasted_iota(jnp.int32, rows.shape, 0)
        records.append(jnp.where(field == 6, state[9, b : b + 1, :], rows))
    filled = jnp.sum(jnp.where(state[9] > 0.0, 1, 0), axis=1, keepdims=True)
    entries = []
    for place in plan.places():
        entry = []
        for n in range(7):
            own, other = plan.neighbour(place, n)
            if own:
                entry.append((records[other], filled[other, 0], neighbours[n]))
        entries.append(entry)
    jobs = list_pairs(plan, entries, packed, table)
    run_pairs(jobs, spread, packed, table, parts)
    if not with_fluid:
        return
    for fetch in fetches:
        fetch.wait()
    slots = radius.shape[-1]
    span = [s // d for s, d in zip(fluid.shape[1:], plan.dims)]
    sub = lax.broadcasted_iota(jnp.int32, (8, slots), 0)
    for place in plan.places():
        b = plan.index(place)
        cell = cells[b : b + 1, :]
        column = jnp.broadcast_to(cell % span[2], (8, slots))
        row = jnp.broadcast_to(cell // span[2], (8, slots)) - sub
        sums_c = [jnp.zeros((8, slots), f32) for c in range(3)]
        for a in range(span[0]):
            for h in range(span[1] // 8):
                hit = row == a * span[1] + h * 8
                y0 = place[1] * span[1] + h * 8
                z0 = place[2] * span[2]
                for c in range(3):
                    block = fluid[c, place[0] * span[0] + a, y0 : y0 + 8, z0 : z0 + span[2]]
                    got = jnp.take_along_axis(block, column, axis=1)
                    sums_c[c] = jnp.where(hit, got, sums_c[c])
        for c in range(3):
            gas[c, b : b + 1, :] = jnp.sum(sums_c[c], axis=0, keepdims=True)


def step_core(plan, sizes, state, radius, spread, inner, springs, partners, gas, halos, out,
              new_springs, around, beside, packed, table, parts):
    scale = normal_damp / normal_stiff
    places = plan.places()
    slots = radius.shape[-1]
    split = per_axis(halos, sizes)
    around[0] = state[...]
    sub = lax.broadcasted_iota(jnp.int32, (plan.count, slots), 0)
    inner_count = [plan.dims[1] * plan.dims[2], plan.dims[2], 1]
    entries = [[] for _ in places]
    parts[...] = inner[...]
    bins = plan.count
    for axis in range(3):
        stride = inner_count[axis]
        dim = plan.dims[axis]
        level = sub // stride % dim
        for f in range(FIELDS):
            rows = slice(f // 2 * bins, (f // 2 + 1) * bins)
            far = (dim - 1 - f % 2) * stride
            got = ordered_receive(AXES[axis], sizes[axis], [ref[rows, :] for ref in split[axis]])
            for side in (-1, 1):
                n = 2 * axis + (1 if side < 0 else 2)
                edge = dim - 1 if side > 0 else 0
                own = pltpu.roll(state[f], -side * stride % bins, 0)
                other = pltpu.roll(got[1 if side > 0 else 0], side * far % bins, 0)
                value = jnp.where(level == edge, other, own)
                if f == 9:
                    gone = at_end(AXES[axis], sizes[axis], side)
                    value = jnp.where(((level == edge) & gone) | (value <= 0.0), DEAD, value)
                    beside[n, :, 6, :] = value
                    beside[n, :, 7, :] = value
                    filled = jnp.sum(jnp.where(value > 0.0, 1, 0), axis=1, keepdims=True)
                    for place in places:
                        if not plan.neighbour(place, n)[0]:
                            b = plan.index(place)
                            entries[b].append((n, filled[b, 0]))
                elif f < 3:
                    beside[n, :, f, :] = value + float(neighbours[n][f])
                elif f < 6:
                    beside[n, :, f, :] = value * scale
                around[n, f] = value
    entries = [
        [(beside[n, b], count, (0, 0, 0)) for n, count in entries[b]] for b in range(bins)
    ]
    jobs = list_pairs(plan, entries, packed, table)
    run_pairs(jobs, spread, packed, table, parts)
    normal = []
    for k in range(3):
        sums = [
            jnp.sum(jnp.transpose(parts[b, k], (1, 0)), axis=0, keepdims=True)
            for b in range(plan.count)
        ]
        normal.append(jnp.concatenate(sums, axis=0) * normal_stiff)
    place_i = [state[k] for k in range(3)]
    speed_i = [state[3 + k] for k in range(3)]
    turn_i = [state[6 + k] for k in range(3)]
    rad_i = radius[...]
    shear_sum = [jnp.zeros_like(rad_i) for k in range(3)]
    twist = [jnp.zeros_like(rad_i) for k in range(3)]
    for h in range(partners.shape[0]):
        code = partners[h]
        valid = code >= 0
        code = jnp.maximum(code, 0)
        which = code // slots
        member = code % slots
        picked = []
        for f in range(FIELDS):
            value = jnp.take_along_axis(around[0, f], member, axis=1)
            for n in range(1, 7):
                got = jnp.take_along_axis(around[n, f], member, axis=1)
                value = jnp.where(which == n, got, value)
            picked.append(value)
        alive = valid & (picked[9] > 0.0)
        sep = []
        for k in range(3):
            shift = jnp.where(which == 2 + 2 * k, 1.0, jnp.where(which == 1 + 2 * k, -1.0, 0.0))
            sep.append(place_i[k] - picked[k] - shift)
        distance = jnp.sqrt(sep[0] * sep[0] + sep[1] * sep[1] + sep[2] * sep[2] + soft_length**2)
        unit = [s / distance for s in sep]
        over = jnp.maximum(rad_i + picked[9] - distance, 0.0)
        root = jnp.sqrt(over)
        rel = [speed_i[k] - picked[3 + k] for k in range(3)]
        approach = rel[0] * unit[0] + rel[1] * unit[1] + rel[2] * unit[2]
        pressing = normal_stiff * over * root - normal_damp * root * approach
        lever = [rad_i * turn_i[k] + picked[9] * picked[6 + k] for k in range(3)]
        contact = [
            rel[k]
            - (
                lever[(k + 1) % 3] * unit[(k + 2) % 3]
                - lever[(k + 2) % 3] * unit[(k + 1) % 3]
            )
            for k in range(3)
        ]
        along = contact[0] * unit[0] + contact[1] * unit[1] + contact[2] * unit[2]
        old = [springs[k, h] for k in range(3)]
        old_along = old[0] * unit[0] + old[1] * unit[1] + old[2] * unit[2]
        stretched = [
            old[k] - old_along * unit[k] + time_step * (contact[k] - along * unit[k])
            for k in range(3)
        ]
        length = jnp.sqrt(
            stretched[0] * stretched[0] + stretched[1] * stretched[1] + stretched[2] * stretched[2]
        )
        limit = jnp.minimum(
            1.0, friction * jnp.abs(pressing) / jnp.maximum(shear_stiff * length, force_floor)
        )
        limit = jnp.where(alive, limit, 0.0)
        fresh = [limit * stretched[k] for k in range(3)]
        for k in range(3):
            new_springs[k, h] = fresh[k]
            shear_sum[k] = shear_sum[k] - shear_stiff * fresh[k]
            twist[k] = twist[k] - shear_stiff * (
                fresh[(k + 1) % 3] * unit[(k + 2) % 3] - fresh[(k + 2) % 3] * unit[(k + 1) % 3]
            )
    safe = jnp.where(rad_i > 0.0, rad_i, 1.0)
    ratio = safe / 0.1
    mass = ratio * ratio * ratio
    inertia = 0.4 * mass * safe * safe
    for k in range(3):
        force = normal[k] + shear_sum[k] + drag_coeff * (gas[k] - speed_i[k])
        lift = gravity if k == 2 else 0.0
        speed = speed_i[k] + time_step * (force / mass - lift)
        out[k] = place_i[k] + time_step * speed
        out[3 + k] = speed
        out[6 + k] = turn_i[k] + time_step * (rad_i * twist[k]) / inertia
    out[9] = state[9]


def middle_kernel(plan, sizes, *refs):
    n = send_count(sizes)
    state, radius, spread, inner, springs, partners, gas, pressure = refs[:8]
    halos = refs[8 : 8 + n]
    out, new_springs = refs[8 + n : 10 + n]
    sends = refs[10 + n : 10 + 2 * n]
    scratch = refs[10 + 2 * n :]
    put_pressure(plan, sizes, radius.shape[-1], pressure, sends)
    step_core(plan, sizes, state, radius, spread, inner, springs, partners, gas, halos, out,
              new_springs, *scratch)
    put_faces(plan, sizes, out, sends)


def last_kernel(plan, sizes, *refs):
    n = send_count(sizes)
    state, radius, spread, inner, springs, partners, gas, departures = refs[:8]
    halos = refs[8 : 8 + n]
    places, speeds, turns, new_springs, out = refs[8 + n : 13 + n]
    sends = refs[13 + n : 13 + 2 * n]
    scratch = refs[13 + 2 * n :]
    step_core(plan, sizes, state, radius, spread, inner, springs, partners, gas, halos, out,
              new_springs, *scratch)
    places[...] = out[0:3]
    speeds[...] = out[3:6]
    turns[...] = out[6:9]
    slots = radius.shape[-1]
    hist = partners.shape[0]
    count = plan.count
    sub = lax.broadcasted_iota(jnp.int32, (count, slots), 0)
    values = [out[f] for f in range(9)] + [radius[...]]
    values += [new_springs[k, h] for k in range(3) for h in range(hist)]
    values += [(partners[h] + 1).astype(f32) for h in range(hist)]
    width = len(values)
    picks = [[], [], [], [], [], []]
    for d in range(6):
        leaving = jnp.broadcast_to(departures[d : d + 1, :], (count, slots))
        hit = (leaving // slots == sub) & (leaving >= 0)
        member = jnp.maximum(leaving, 0) % slots
        for v in values:
            got = jnp.where(hit, jnp.take_along_axis(v, member, axis=1), 0.0)
            picks[d].append(jnp.sum(got, axis=0, keepdims=True))
    split = per_axis(sends, sizes)
    for axis in range(3):
        for f in range(width):
            blocks = ordered_send(
                AXES[axis], sizes[axis], picks[2 * axis][f], picks[2 * axis + 1][f]
            )
            for ref, block in zip(split[axis], blocks):
                ref[f : f + 1, :] = block


def deposit_kernel(plan, sizes, *refs):
    n = send_count(sizes)
    state, radius, cells, gas, pressure, source = refs[:6]
    halos = refs[6 : 6 + n]
    force_out, pressure_out, force, new_pressure, sems = refs[6 + n :]
    copies = []

    def send(source, target):
        copies.append(pltpu.make_async_copy(source, target, sems.at[len(copies)]))
        copies[-1].start()

    slots = radius.shape[-1]
    nx, ny, nz = pressure.shape
    lanes = slots
    chunks = nz // lanes
    span = [s // d for s, d in zip(pressure.shape, plan.dims)]
    rows = span[0] * span[1]
    high_row = lax.broadcasted_iota(jnp.int32, (rows, slots), 0)
    column_row = lax.broadcasted_iota(jnp.int32, (span[2], slots), 0)
    def deposit(place):
        b = plan.index(place)
        cell = cells[b : b + 1, :]
        live = state[9, b : b + 1, :] > 0.0
        rad = radius[b : b + 1, :]
        values = [
            jnp.where(live, drag_coeff * (state[3 + c, b : b + 1, :] - gas[c, b : b + 1, :]), 0.0)
            for c in range(3)
        ]
        values.append(jnp.where(live, 4.0 / 3.0 * math.pi * rad * rad * rad, 0.0))
        at_row = high_row == cell // span[2]
        at_column = (column_row == cell % span[2]).astype(jnp.bfloat16)
        halves = []
        for v in values:
            top = v.astype(jnp.bfloat16).astype(f32)
            left = v - top
            halves.append(
                jnp.concatenate(
                    [jnp.where(at_row, part, 0.0).astype(jnp.bfloat16) for part in (top, left)],
                    axis=1,
                )
            )
        left = jnp.concatenate(halves, axis=0)
        right = jnp.concatenate([at_column] * 2, axis=1)
        got = lax.dot_general(
            left, right, (((1,), (1,)), ((), ())), preferred_element_type=f32
        )
        x0, y0, z0 = (p * s for p, s in zip(place, span))
        block = (slice(x0, x0 + span[0]), slice(y0, y0 + span[1]), slice(z0, z0 + span[2]))
        pieces = [got[c * rows : (c + 1) * rows].reshape(span) for c in range(4)]
        for c in range(3):
            force[(c,) + block] = pieces[c]
        new_pressure[block] = volume_coeff * pieces[3] + pieces[2]
    split = per_axis(halos, sizes)
    dead = [
        [at_end(AXES[axis], sizes[axis], side) for side in (-1, 1)] for axis in range(3)
    ]
    base = FIELDS // 2 * plan.count
    slabs = []
    for ref in split[0]:
        slabs.append(
            jnp.concatenate(
                [ref[base + c * ny : base + (c + 1) * ny, :] for c in range(chunks)], axis=1
            )
        )
    x_ends = ordered_receive("gx", sizes[0], slabs)
    x_ends = [jnp.where(dead[0][s], 0.0, x_ends[s]) for s in (0, 1)]
    base = FIELDS // 2 * plan.count
    slabs = []
    for ref in split[1]:
        slabs.append(
            jnp.concatenate(
                [ref[base + c * nx : base + (c + 1) * nx, :] for c in range(chunks)], axis=1
            )
        )
    y_ends = ordered_receive("gy", sizes[1], slabs)
    y_ends = [jnp.where(dead[1][s], 0.0, y_ends[s]) for s in (0, 1)]
    base = FIELDS // 2 * plan.count
    z_ends = ordered_receive("gz", sizes[2], [ref[base : base + ny, :] for ref in split[2]])
    z_ends = [jnp.where(dead[2][s], 0.0, z_ends[s]) for s in (0, 1)]
    row = lax.broadcasted_iota(jnp.int32, (ny, nz), 0)
    column = lax.broadcasted_iota(jnp.int32, (ny, nz), 1)
    def sweep(x):
        here = pressure[x]
        total = pressure[x - 1] if x > 0 else x_ends[0]
        total = total + (pressure[x + 1] if x < nx - 1 else x_ends[1])
        total = total + jnp.where(row == 0, y_ends[0][x : x + 1, :], pltpu.roll(here, 1, 0))
        total = total + jnp.where(
            row == ny - 1, y_ends[1][x : x + 1, :], pltpu.roll(here, ny - 1, 0)
        )
        total = total + jnp.where(column == 0, z_ends[0][:, x : x + 1], pltpu.roll(here, 1, 1))
        total = total + jnp.where(
            column == nz - 1, z_ends[1][:, x : x + 1], pltpu.roll(here, nz - 1, 1)
        )
        new_pressure[x] = (total + (source[x] + new_pressure[x])) * (1.0 / 6.0)

    layers = plan.dims[0]
    for layer in range(layers + 1):
        if layer < layers:
            for place in plan.places():
                if place[0] == layer:
                    deposit(place)
        if layer > 0:
            for x in range((layer - 1) * span[0], layer * span[0]):
                sweep(x)
        if layer < layers:
            part = slice(layer * span[0], (layer + 1) * span[0])
            for c in range(3):
                send(force.at[c, part], force_out.at[c, part])
        if layer > 0:
            part = slice((layer - 1) * span[0], layer * span[0])
            send(new_pressure.at[part], pressure_out.at[part])
    for copy in copies:
        copy.wait()


def arrive_kernel(sizes, *refs):
    n = send_count(sizes)
    halos = refs[:n]
    state, codes = refs[n:]
    split = per_axis(halos, sizes)
    width = state.shape[0]
    hist = codes.shape[1]
    for axis in range(3):
        got = [ref[0 : width + hist, :] for ref in split[axis]]
        before, after = ordered_receive(AXES[axis], sizes[axis], got)
        after = jnp.where(at_end(AXES[axis], sizes[axis], 1), 0.0, after)
        before = jnp.where(at_end(AXES[axis], sizes[axis], -1), 0.0, before)
        for d, block in ((2 * axis, after), (2 * axis + 1, before)):
            state[:, d, 0, :] = block[0:width]
            codes[d] = block[width : width + hist].astype(jnp.int32) - 1


def call(kernel, outs, scratch, args, hbm=(), flops=0, outs_hbm=False):
    specs = []
    args = [
        pltpu.with_memory_space_constraint(a, pltpu.HBM) if k in hbm else a
        for k, a in enumerate(args)
    ]
    for k in range(len(args)):
        space = pltpu.HBM if k in hbm else pltpu.VMEM
        specs.append(pl.BlockSpec(memory_space=space))
    return pl.pallas_call(
        kernel,
        out_shape=[jax.ShapeDtypeStruct(s, d) for s, d in outs],
        in_specs=specs,
        out_specs=[pl.BlockSpec(memory_space=pltpu.HBM if outs_hbm else pltpu.VMEM)] * len(outs),
        scratch_shapes=scratch,
        compiler_params=pltpu.CompilerParams(vmem_limit_bytes=32 * 1024 * 1024),
        cost_estimate=pl.CostEstimate(flops=flops, bytes_accessed=1 << 20, transcendentals=0),
    )(*args)


def body(sizes, positions, velocities, spins, radii, counts, springs, partners, cells, departures,
         fluid_velocity, pressure, pressure_source):
    plan = Plan(radii.shape[:3])
    count = plan.count
    slots = radii.shape[3]
    hist = partners.shape[0]
    nx, ny, nz = pressure.shape
    chunks = nz // slots
    flat = lambda a: a.reshape(a.shape[:-4] + (count, slots))
    pos, vel, spin = flat(positions), flat(velocities), flat(spins)
    radius = radii.reshape(count, slots)
    springs = springs.reshape(3, hist, count, slots)
    partners = partners.reshape(hist, count, slots)
    cells = cells.reshape(count, slots)
    leaving = departures.reshape(6, slots)

    faces = [FIELDS // 2 * count] * 3
    extra = [chunks * ny, chunks * nx, ny]
    vm = lambda *s: pltpu.VMEM(s, f32)

    def sends(rows):
        out = []
        for a in range(3):
            for _ in rolls(AXES[a], sizes):
                out.append(((rows[a], slots), f32))
        return [out[k] for k in start_order(sizes)]

    inside = [sum(plan.neighbour(p, n)[0] for n in range(7)) for p in plan.places()]

    def pair_scratch(jobs):
        return [vm(jobs + 2, 8, slots), pltpu.SMEM((jobs + 8,), jnp.int32)]

    own_scratch = [vm(count, 8, slots)] + pair_scratch(sum(inside))
    spread_shape = ((count, 7, slots, slots), f32)
    parts_shape = ((count, 3, slots, slots), f32)
    step_scratch = [vm(7, FIELDS, count, slots), vm(7, count, 8, slots)] + pair_scratch(7 * count - sum(inside))
    step_scratch.append(vm(count, 3, slots, slots))
    state_shape = ((FIELDS, count, slots), f32)
    three = ((3, count, slots), f32)
    spring_shape = ((3, hist, count, slots), f32)
    bind = functools.partial

    state, radius, *out = call(
        bind(pack_kernel, plan, sizes),
        [state_shape, ((count, slots), f32)] + sends(faces),
        [
            pltpu.VMEM(counts.shape, jnp.int32),
            pltpu.SemaphoreType.DMA((5,)),
        ],
        [pos, vel, spin, radius, counts],
        hbm=(0, 1, 2, 3, 4),
        flops=1 << 20,
    )
    first_halos = exchange(out, sizes)
    spread, inner, gas, cells = call(
        bind(inner_kernel, plan, True),
        [spread_shape, parts_shape, three, ((count, slots), jnp.int32)],
        own_scratch + [vm(3, nx, ny, nz), pltpu.SemaphoreType.DMA((2,))],
        [state, radius, cells, fluid_velocity],
        hbm=(2, 3),
        flops=1 << 25,
    )
    state, springs, *out = call(
        bind(middle_kernel, plan, sizes),
        [state_shape, spring_shape] + sends([f + e for f, e in zip(faces, extra)]),
        step_scratch,
        [state, radius, spread, inner, springs, partners, gas, pressure] + first_halos,
        flops=1 << 25,
    )
    halos = exchange(out, sizes)
    spread, inner = call(
        bind(inner_kernel, plan, False), [spread_shape, parts_shape], own_scratch,
        [state, radius], flops=1 << 25
    )
    width = 10 + 4 * hist
    padded = (width + 7) // 8 * 8
    places, speeds, turns, springs, state, *out = call(
        bind(last_kernel, plan, sizes),
        [three, three, three, spring_shape, state_shape] + sends([padded] * 3),
        step_scratch,
        [state, radius, spread, inner, springs, partners, gas, leaving] + halos,
        flops=1 << 25,
    )
    arrivals = exchange(out, sizes)
    force, new_pressure = call(
        bind(deposit_kernel, plan, sizes),
        [((3, nx, ny, nz), f32), ((nx, ny, nz), f32)],
        [
            vm(3, nx, ny, nz),
            vm(nx, ny, nz),
            pltpu.SemaphoreType.DMA((4 * plan.dims[0],)),
        ],
        [state, radius, cells, gas, pressure, pressure_source] + halos,
        outs_hbm=True,
        flops=1 << 25,
    )
    arrived, arrived_partners = call(
        bind(arrive_kernel, sizes),
        [((10 + 3 * hist, 6, 1, slots), f32), ((6, hist, slots), jnp.int32)],
        [],
        arrivals,
        flops=1 << 20,
    )
    wide = lambda a: a.reshape(a.shape[:-2] + radii.shape)
    return (
        wide(places),
        wide(speeds),
        wide(turns),
        wide(springs),
        force,
        new_pressure,
        arrived.reshape(1, 1, 1, 10 + 3 * hist, 6, slots),
        jnp.transpose(arrived_partners, (1, 0, 2))[None, None, None],
    )


def solution(mesh):
    sizes = tuple(mesh.shape[a] for a in AXES)
    return jax.shard_map(
        functools.partial(body, sizes),
        mesh=mesh,
        in_specs=(
            P(None, "gx", "gy", "gz", None),
            P(None, "gx", "gy", "gz", None),
            P(None, "gx", "gy", "gz", None),
            P("gx", "gy", "gz", None),
            P("gx", "gy", "gz"),
            P(None, None, "gx", "gy", "gz", None),
            P(None, "gx", "gy", "gz", None),
            P("gx", "gy", "gz", None),
            P("gx", "gy", "gz", None, None),
            P(None, "gx", "gy", "gz"),
            P("gx", "gy", "gz"),
            P("gx", "gy", "gz"),
        ),
        out_specs=(
            P(None, "gx", "gy", "gz", None),
            P(None, "gx", "gy", "gz", None),
            P(None, "gx", "gy", "gz", None),
            P(None, None, "gx", "gy", "gz", None),
            P(None, "gx", "gy", "gz"),
            P("gx", "gy", "gz"),
            P("gx", "gy", "gz", None, None, None),
            P("gx", "gy", "gz", None, None, None),
        ),
        check_vma=False,
    )
```
